128 devices in a mesh: data: 4 (over z), col: 4 (over y), row: 8 (over x, core).
Axes of the slice: x: 4, y: 4, z: 4, core: 2. Of those that a mesh axis runs over, the one named last changes fastest.
Arguments:
- x_in: bfloat16 [4096, 3072], P(None, 'row')
- h_act: bfloat16 [4096, 8192], P(None, 'row')
- d_gate: bfloat16 [4096, 8192], P(None, 'col')
- d_up: bfloat16 [4096, 8192], P(None, 'col')
- d_out: bfloat16 [4096, 3072], P(None, 'col')
- w_gate: float32 [3072, 8192], P('row', 'col')
- w_up: float32 [3072, 8192], P('row', 'col')
- w_down: float32 [8192, 3072], P('row', 'col')
- r_gate: float32 [3072], P('row')
- c_gate: float32 [8192], P('col')
- r_up: float32 [3072], P('row')
- c_up: float32 [8192], P('col')
- r_down: float32 [8192], P('row')
- c_down: float32 [3072], P('col')
- beta_two: float32 [], replicated
- rel_step: float32 [], replicated
- clip_thr: float32 [], replicated
Outputs:
- output 1: float32 [3072, 8192], P('row', 'col')
- output 2: float32 [3072, 8192], P('row', 'col')
- output 3: float32 [8192, 3072], P('row', 'col')
- output 4: float32 [3072], P('row')
- output 5: float32 [8192], P('col')
- output 6: float32 [3072], P('row')
- output 7: float32 [8192], P('col')
- output 8: float32 [8192], P('row')
- output 9: float32 [3072], P('col')
All inputs are finite; a program needn't handle non-finite values.
Results may differ from the reference program's by a relative error of at most 0.001.
Values are sent between devices in bfloat16 or wider.
A program may use at most 1 GiB of HBM per device.

```python
import jax
import jax.numpy as jnp

TOKENS = 4096
D = 3072
FF = 8192

EPS_SQ = 1e-30
EPS_SCALE = 1e-3
DOWN_STAT_SCALE = 60.0


def weight_grad(act_in, cot_out):
    return jnp.dot(act_in.T, cot_out, preferred_element_type=jnp.float32)


def adafactor_step(w_mat, g_mat, r_old, c_old, beta_two, rel_step, clip_thr):
    q_mat = g_mat * g_mat + EPS_SQ
    r_new = beta_two * r_old + (1.0 - beta_two) * jnp.mean(q_mat, axis=1)
    c_new = beta_two * c_old + (1.0 - beta_two) * jnp.mean(q_mat, axis=0)
    v_mat = r_new[:, None] * c_new[None, :] / jnp.mean(r_new)
    u_mat = g_mat / jnp.sqrt(v_mat)
    u_rms = jnp.sqrt(jnp.mean(u_mat * u_mat))
    u_hat = u_mat / jnp.maximum(1.0, u_rms / clip_thr)
    w_rms = jnp.sqrt(jnp.mean(w_mat * w_mat))
    step_size = rel_step * jnp.maximum(EPS_SCALE, w_rms)
    return w_mat - step_size * u_hat, r_new, c_new


def old_stats(g_mat, key_row, key_col, stat_scale):
    q_mat = g_mat * g_mat
    row_fac = jnp.exp(jax.random.uniform(key_row, (g_mat.shape[0],), jnp.float32, -1.2, 1.2))
    col_fac = jnp.exp(jax.random.uniform(key_col, (g_mat.shape[1],), jnp.float32, -1.2, 1.2))
    return stat_scale * jnp.mean(q_mat, axis=1) * row_fac, stat_scale * jnp.mean(q_mat, axis=0) * col_fac


def setup_inputs(seed: int = 0) -> dict:
    key_list = jax.random.split(jax.random.key(seed), 17)
    x_in = jax.random.normal(key_list[0], (TOKENS, D), jnp.float32).astype(jnp.bfloat16)
    h_act = jax.random.normal(key_list[1], (TOKENS, FF), jnp.float32).astype(jnp.bfloat16)
    d_gate = jax.random.normal(key_list[2], (TOKENS, FF), jnp.float32).astype(jnp.bfloat16)
    d_up = jax.random.normal(key_list[3], (TOKENS, FF), jnp.float32).astype(jnp.bfloat16)
    d_out = jax.random.normal(key_list[4], (TOKENS, D), jnp.float32).astype(jnp.bfloat16)
    w_gate = jax.random.normal(key_list[5], (D, FF), jnp.float32) * D ** -0.5
    w_up = jax.random.normal(key_list[6], (D, FF), jnp.float32) * D ** -0.5
    w_down = jax.random.normal(key_list[7], (FF, D), jnp.float32) * FF ** -0.5
    r_gate, c_gate = old_stats(weight_grad(x_in, d_gate), key_list[8], key_list[9], 1.0)
    r_up, c_up = old_stats(weight_grad(x_in, d_up), key_list[10], key_list[11], 1.0)
    r_down, c_down = old_stats(weight_grad(h_act, d_out), key_list[12], key_list[13], DOWN_STAT_SCALE)
    beta_two = jax.random.uniform(key_list[14], (), jnp.float32, 0.5, 0.9)
    rel_step = jax.random.uniform(key_list[15], (), jnp.float32, 0.2, 0.6)
    clip_thr = jax.random.uniform(key_list[16], (), jnp.float32, 0.4, 0.6)
    return dict(x_in=x_in, h_act=h_act, d_gate=d_gate, d_up=d_up, d_out=d_out, w_gate=w_gate, w_up=w_up, w_down=w_down, r_gate=r_gate, c_gate=c_gate, r_up=r_up, c_up=c_up, r_down=r_down, c_down=c_down, beta_two=beta_two, rel_step=rel_step, clip_thr=clip_thr)


def reference(x_in, h_act, d_gate, d_up, d_out, w_gate, w_up, w_down, r_gate, c_gate, r_up, c_up, r_down, c_down, beta_two, rel_step, clip_thr):
    gate_w, gate_r, gate_c = adafactor_step(w_gate, weight_grad(x_in, d_gate), r_gate, c_gate, beta_two, rel_step, clip_thr)
    up_w, up_r, up_c = adafactor_step(w_up, weight_grad(x_in, d_up), r_up, c_up, beta_two, rel_step, clip_thr)
    down_w, down_r, down_c = adafactor_step(w_down, weight_grad(h_act, d_out), r_down, c_down, beta_two, rel_step, clip_thr)
    return (gate_w, up_w, down_w, gate_r, gate_c, up_r, up_c, down_r, down_c)
```

```python
import functools

import jax
import jax.numpy as jnp
from jax import lax
from jax.experimental import pallas as pl
from jax.experimental.pallas import tpu as pltpu
from jax.sharding import PartitionSpec as P

F32 = jnp.float32
BF16 = jnp.bfloat16
MESH = pl.DeviceIdType.MESH
EPS_SQ = 1e-30
EPS_SCALE = 1e-3
LANES = 128
CONTRACT_TOKENS = (((0,), (0,)), ((), ()))
VMEM_SPEC = pl.BlockSpec(memory_space=pltpu.VMEM)
HBM_SPEC = pl.BlockSpec(memory_space=pltpu.HBM)
SMEM_SPEC = pl.BlockSpec(memory_space=pltpu.SMEM)

DOWN_STEPS = (1, 1, 2, 4)
GATE_STEPS = (4, 4)
UP_STEPS = (4, 4)


def token_dot(act, cot):
    return lax.dot_general(act, cot, CONTRACT_TOKENS, preferred_element_type=F32)


def lane_groups(value):
    parts = [value[:, k : k + LANES] for k in range(0, value.shape[1], LANES)]
    while len(parts) > 1:
        parts = [sum(parts[k : k + 2]) for k in range(0, len(parts), 2)]
    return parts[0]


def update_kernel(row_count, col_count, x_hbm, h_hbm, dg_hbm, du_hbm, do_hbm, wg_hbm, wu_hbm, wd_hbm, rg, cg, ru, cu, rd, cd, beta_ref, step_ref, clip_ref,
                  g_gate, g_up, g_down, w_gate, w_up, w_down, a_gate, a_up, a_down, b_gate, b_up, b_down, rn_gate, cn_gate, rn_up, cn_up, rn_down, cn_down,
                  x_buf, gate_buf, mix_buf, row_gate, row_up, row_down, col_gate, col_up, col_down, tail_buf,
                  load_sem, w_sem, row_send, row_recv, col_send, col_recv, tail_send, tail_recv):
    row_me = lax.axis_index("row")
    col_me = lax.axis_index("col")
    plane = row_count * col_count
    tokens = x_hbm.shape[0]
    unit = tokens // 8
    h_cols = h_hbm.shape[1]
    do_cols = do_hbm.shape[1]

    def row_peer(k):
        return lax.rem(row_me + k, row_count)

    def col_peer(k):
        return lax.rem(col_me + k, col_count)

    barrier = pltpu.get_barrier_semaphore()
    for dc in range(col_count):
        for dr in range(row_count):
            if dc or dr:
                pl.semaphore_signal(barrier, inc=1, device_id={"col": col_peer(dc), "row": row_peer(dr)}, device_id_type=MESH)

    loads = []
    step_no = 0

    def add_steps(steps, make):
        nonlocal step_no
        out = []
        at = 0
        for size in steps:
            lo, n = at * unit, size * unit
            copies = [pltpu.make_async_copy(src.at[pl.ds(lo, n), :], dst, load_sem.at[step_no, k]) for k, (src, dst) in enumerate(make(lo, n))]
            out.append((lo, n, copies))
            loads.append(copies)
            step_no += 1
            at += size
        return out

    down = add_steps(DOWN_STEPS, lambda lo, n: [(h_hbm, mix_buf.at[pl.ds(lo, n), pl.ds(0, h_cols)]), (do_hbm, mix_buf.at[pl.ds(lo, n), pl.ds(h_cols, do_cols)])])
    gate = add_steps(GATE_STEPS, lambda lo, n: [(x_hbm, x_buf.at[pl.ds(lo, n), :]), (dg_hbm, gate_buf.at[pl.ds(lo, n), :])])
    up = add_steps(UP_STEPS, lambda lo, n: [(du_hbm, mix_buf.at[pl.ds(lo, n), :])])
    w_copies = [pltpu.make_async_copy(src, dst, w_sem.at[k]) for k, (src, dst) in enumerate(((wd_hbm, w_down), (wg_hbm, w_gate), (wu_hbm, w_up)))]

    def start(copies):
        for copy in copies:
            copy.start()

    def wait(copies):
        for copy in copies:
            copy.wait()

    def exchange(kind, buf, own, send_sem, recv_sem, index):
        count, me = (col_count, col_me) if kind == "col" else (row_count, row_me)
        peer = col_peer if kind == "col" else row_peer
        buf[pl.ds(me, 1)] = own[None]
        for k in range(1, count):
            pltpu.make_async_remote_copy(buf.at[me], buf.at[me], send_sem.at[index], recv_sem.at[index], device_id={kind: peer(k)}, device_id_type=MESH).start()

        def finish():
            pltpu.make_async_copy(buf.at[pl.ds(0, count - 1)], buf.at[pl.ds(0, count - 1)], send_sem.at[index]).wait()
            pltpu.make_async_copy(buf.at[pl.ds(0, count - 1)], buf.at[pl.ds(0, count - 1)], recv_sem.at[index]).wait()
        return finish

    def sums_out(g, row_buf, col_buf, index):
        q = g * g
        col_part = jnp.sum(q, axis=0, keepdims=True) + q.shape[0] * EPS_SQ
        row_part = jnp.sum(lane_groups(q).T, axis=0, keepdims=True) + q.shape[1] * EPS_SQ
        first = exchange("row", col_buf, col_part, col_send, col_recv, index)
        second = exchange("col", row_buf, row_part, row_send, row_recv, index)
        return first, second

    beta = beta_ref[0]

    def new_stats(finish, g_ref, row_buf, col_buf, r_old, c_old, r_new, c_new, a_ref, b_ref):
        for part in finish:
            part()
        m_total = g_ref.shape[0] * row_count
        n_total = g_ref.shape[1] * col_count
        row_sum = sum(row_buf[k] for k in range(1, col_count)) + row_buf[0]
        col_sum = sum(col_buf[k] for k in range(1, row_count)) + col_buf[0]
        r_val = beta * r_old[...] + (1.0 - beta) * (row_sum / n_total)
        c_val = beta * c_old[...] + (1.0 - beta) * (col_sum / m_total)
        r_new[...] = r_val
        c_new[...] = c_val
        a_row = 1.0 / jnp.sqrt(r_val)
        b_row = 1.0 / jnp.sqrt(c_val)
        a_col = jnp.broadcast_to(a_row, (LANES, a_row.shape[1])).T
        a_ref[...] = a_col
        b_ref[...] = b_row
        t = g_ref[...] * b_row
        u_rows = lane_groups(t * t) * (a_col * a_col)
        return jnp.sum(u_rows, axis=0, keepdims=True), lane_groups(r_val)

    def square_sum(w_ref):
        w = w_ref[...]
        return jnp.sum(lane_groups(w * w), axis=0, keepdims=True)

    for copies in loads[: len(down) + 1]:
        start(copies)

    def matmul(steps, g_ref, act, cot, after):
        for k, (lo, n, copies) in enumerate(steps):
            wait(copies)
            part = token_dot(act(lo, n), cot(lo, n))
            total = part if k == 0 else g_ref[...] + part
            g_ref[...] = total
            after(k)
        return total

    def after_down(k):
        if k == len(down) - 1:
            for item in gate[1:] + up:
                start(item[2])
            start(w_copies)

    total = matmul(down, g_down, lambda lo, n: mix_buf[pl.ds(lo, n), 0:h_cols], lambda lo, n: mix_buf[pl.ds(lo, n), h_cols : h_cols + do_cols], after_down)
    pl.semaphore_wait(barrier, plane - 1)
    down_out = sums_out(total, row_down, col_down, 0)
    total = matmul(gate, g_gate, lambda lo, n: x_buf[pl.ds(lo, n), :], lambda lo, n: gate_buf[pl.ds(lo, n), :], lambda k: None)
    gate_out = sums_out(total, row_gate, col_gate, 1)
    total = matmul(up, g_up, lambda lo, n: x_buf[pl.ds(lo, n), :], lambda lo, n: mix_buf[pl.ds(lo, n), :], lambda k: None)
    up_out = sums_out(total, row_up, col_up, 2)

    wait(w_copies)
    w_sums = [square_sum(w) for w in (w_down, w_gate, w_up)]
    u_down, r_down = new_stats(down_out, g_down, row_down, col_down, rd, cd, rn_down, cn_down, a_down, b_down)
    u_gate, r_gate = new_stats(gate_out, g_gate, row_gate, col_gate, rg, cg, rn_gate, cn_gate, a_gate, b_gate)
    u_up, r_up = new_stats(up_out, g_up, row_up, col_up, ru, cu, rn_up, cn_up, a_up, b_up)

    lane = lax.broadcasted_iota(jnp.int32, (1, LANES), 1)
    packed = jnp.zeros((1, LANES), F32)
    for k, value in enumerate(w_sums + [r_down, r_gate, r_up, u_down, u_gate, u_up]):
        packed = jnp.where(lane == k, jnp.sum(value, axis=1, keepdims=True), packed)
    me = col_me * row_count + row_me
    tail_buf[pl.ds(me, 1)] = packed[None]
    for dc in range(col_count):
        for dr in range(row_count):
            if dc or dr:
                pltpu.make_async_remote_copy(tail_buf.at[me], tail_buf.at[me], tail_send, tail_recv, device_id={"col": col_peer(dc), "row": row_peer(dr)}, device_id_type=MESH).start()
    pltpu.make_async_copy(tail_buf.at[pl.ds(0, plane - 1)], tail_buf.at[pl.ds(0, plane - 1)], tail_send).wait()
    pltpu.make_async_copy(tail_buf.at[pl.ds(0, plane - 1)], tail_buf.at[pl.ds(0, plane - 1)], tail_recv).wait()
    sums = jnp.sum(tail_buf[...], axis=0)

    def pick(k):
        return jnp.sum(jnp.where(lane == k, sums, 0.0), axis=1, keepdims=True)

    for k, (g_ref, a_ref) in enumerate(((g_down, a_down), (g_gate, a_gate), (g_up, a_up))):
        m_total = g_ref.shape[0] * row_count
        n_total = g_ref.shape[1] * col_count
        r_mean = pick(3 + k) / (m_total * col_count)
        w_rms = jnp.sqrt(pick(k) / (m_total * n_total))
        u_rms = jnp.sqrt(r_mean * pick(6 + k) / (m_total * n_total))
        size = step_ref[0] * jnp.maximum(EPS_SCALE, w_rms)
        scale = size * jnp.sqrt(r_mean) / jnp.maximum(1.0, u_rms / clip_ref[0])
        a_ref[...] = a_ref[...] * scale


def apply_kernel(g_gate, g_up, g_down, w_gate, w_up, w_down, a_gate, a_up, a_down, b_gate, b_up, b_down, rn_gate, cn_gate, rn_up, cn_up, rn_down, cn_down,
                 o_gate, o_up, o_down, ro_gate, co_gate, ro_up, co_up, ro_down, co_down, t_gate, t_up, t_down, w_sem, s_sem):
    small = [pltpu.make_async_copy(src, dst, s_sem.at[k]) for k, (src, dst) in enumerate(((rn_gate, ro_gate), (cn_gate, co_gate), (rn_up, ro_up), (cn_up, co_up), (rn_down, ro_down), (cn_down, co_down)))]
    for copy in small:
        copy.start()
    copies = []
    for k, (g, w, a, b, t, o) in enumerate(((g_down, w_down, a_down, b_down, t_down, o_down), (g_gate, w_gate, a_gate, b_gate, t_gate, o_gate), (g_up, w_up, a_up, b_up, t_up, o_up))):
        rows, columns = g.shape
        size = rows // 4
        for part in range(4):
            s = pl.ds(part * size, size)
            a_val = a[s, :]
            for c in range(0, columns, LANES):
                ls = pl.ds(c, LANES)
                t[s, ls] = w[s, ls] - g[s, ls] * (a_val * b[:, ls])
            copy = pltpu.make_async_copy(t.at[s, :], o.at[s, :], w_sem.at[k, part])
            copy.start()
            copies.append(copy)
    for copy in copies + small:
        copy.wait()


def solution(mesh):
    row_count = mesh.shape["row"]
    col_count = mesh.shape["col"]

    def local_program(x_in, h_act, d_gate, d_up, d_out, w_gate, w_up, w_down, r_gate, c_gate, r_up, c_up, r_down, c_down, beta_two, rel_step, clip_thr):
        vec = lambda v: v.reshape(1, -1)
        blocks = (w_gate, w_up, w_down)
        tokens = x_in.shape[0]
        steps = len(DOWN_STEPS) + len(GATE_STEPS) + len(UP_STEPS)
        out_shape = [pltpu.VMEM(w.shape, F32) for w in blocks] * 2
        out_shape += [pltpu.VMEM((w.shape[0], LANES), F32) for w in blocks]
        out_shape += [pltpu.VMEM((1, w.shape[1]), F32) for w in blocks]
        stats = [pltpu.VMEM((1, w.shape[k]), F32) for w in blocks for k in range(2)]
        dma = pltpu.SemaphoreType.DMA
        flops = sum(2 * tokens * w.shape[0] * w.shape[1] for w in blocks)
        mid = pl.pallas_call(
            functools.partial(update_kernel, row_count, col_count),
            out_shape=out_shape + stats,
            in_specs=[HBM_SPEC] * 8 + [VMEM_SPEC] * 6 + [SMEM_SPEC] * 3,
            out_specs=[VMEM_SPEC] * 18,
            scratch_shapes=[
                pltpu.VMEM(x_in.shape, BF16),
                pltpu.VMEM(d_gate.shape, BF16),
                pltpu.VMEM((tokens, max(d_up.shape[1], h_act.shape[1] + d_out.shape[1])), BF16),
                *[pltpu.VMEM((col_count, 1, w.shape[0]), F32) for w in blocks],
                *[pltpu.VMEM((row_count, 1, w.shape[1]), F32) for w in blocks],
                pltpu.VMEM((row_count * col_count, 1, LANES), F32),
                dma((steps, 2)), dma((3,)), dma((3,)), dma((3,)), dma((3,)), dma((3,)), dma, dma,
            ],
            compiler_params=pltpu.CompilerParams(collective_id=0, has_side_effects=True, vmem_limit_bytes=VMEM_A),
            cost_estimate=pl.CostEstimate(flops=flops, bytes_accessed=60_000_000, transcendentals=0),
            name="grad_and_stats",
        )(x_in, h_act, d_gate, d_up, d_out, w_gate, w_up, w_down, vec(r_gate), vec(c_gate), vec(r_up), vec(c_up), vec(r_down), vec(c_down), vec(beta_two)[0], vec(rel_step)[0], vec(clip_thr)[0])
        out = pl.pallas_call(
            apply_kernel,
            out_shape=[jax.ShapeDtypeStruct(w.shape, F32) for w in blocks] + [jax.ShapeDtypeStruct((1, w.shape[k]), F32) for w in blocks for k in range(2)],
            in_specs=[VMEM_SPEC] * 18,
            out_specs=[HBM_SPEC] * 9,
            scratch_shapes=[pltpu.VMEM(w.shape, F32) for w in blocks] + [dma((3, 4)), dma((6,))],
            compiler_params=pltpu.CompilerParams(vmem_limit_bytes=VMEM_B),
            cost_estimate=pl.CostEstimate(flops=10_000_000, bytes_accessed=10_000_000, transcendentals=0),
            name="apply_update",
        )(*mid)
        return tuple(out[:3]) + tuple(v.reshape(-1) for v in out[3:])

    act_spec = P(None, "row")
    cot_spec = P(None, "col")
    w_spec = P("row", "col")
    r_spec = P("row")
    c_spec = P("col")
    s_spec = P()
    return jax.shard_map(local_program, mesh=mesh, in_specs=(act_spec, act_spec, cot_spec, cot_spec, cot_spec, w_spec, w_spec, w_spec, r_spec, c_spec, r_spec, c_spec, r_spec, c_spec, s_spec, s_spec, s_spec), out_specs=(w_spec, w_spec, w_spec, r_spec, c_spec, r_spec, c_spec, r_spec, c_spec), check_vma=False)


VMEM_A = 44 * 2**20
VMEM_B = 14 * 2**20
```

```python
import functools

import jax
import jax.numpy as jnp
from jax import lax
from jax.experimental import pallas as pl
from jax.experimental.pallas import tpu as pltpu
from jax.sharding import PartitionSpec as P

F32 = jnp.float32
BF16 = jnp.bfloat16
MESH = pl.DeviceIdType.MESH
EPS_SQ = 1e-30
EPS_SCALE = 1e-3
LANES = 128
SUBLANES = 8
CHUNKS = 4
CONTRACT_TOKENS = (((0,), (0,)), ((), ()))
VMEM_SPEC = pl.BlockSpec(memory_space=pltpu.VMEM)
HBM_SPEC = pl.BlockSpec(memory_space=pltpu.HBM)
SMEM_SPEC = pl.BlockSpec(memory_space=pltpu.SMEM)
VMEM_A = 44 * 2**20
VMEM_B = 14 * 2**20


def token_dot(act, cot):
    return lax.dot_general(act, cot, CONTRACT_TOKENS, preferred_element_type=F32)


def tree_sum(parts):
    while len(parts) > 1:
        parts = [sum(parts[k + 1 : k + 2], parts[k]) for k in range(0, len(parts), 2)]
    return parts[0]


def lane_groups(value):
    return tree_sum([value[:, k : k + LANES] for k in range(0, value.shape[1], LANES)])


def row_groups(value):
    return tree_sum([value[k : k + SUBLANES] for k in range(0, value.shape[0], SUBLANES)])


def tile_rows(ref):
    return 32 if ref.shape[1] > 1024 else 64


def over_rows(ref, body, init):
    size = tile_rows(ref)
    return lax.fori_loop(0, ref.shape[0] // size, lambda i, carry: body(pl.ds(pl.multiple_of(i * size, size), size), carry), init)


def update_kernel(row_count, col_count, x_hbm, h_hbm, dg_hbm, du_hbm, do_hbm, wg_hbm, wu_hbm, wd_hbm, rg, cg, ru, cu, rd, cd, beta_ref, step_ref, clip_ref,
                  g_gate, g_up, g_down, w_gate, w_up, w_down, a_gate, a_up, a_down, b_gate, b_up, b_down, rn_gate, cn_gate, rn_up, cn_up, rn_down, cn_down,
                  x_buf, gate_buf, mix_buf, row_gate, row_up, row_down, col_gate, col_up, col_down, tail_buf,
                  old_gate_r, old_gate_c, old_up_r, old_up_c, old_down_r, old_down_c, load_sem, w_sem, small_sem, row_send, row_recv, col_send, col_recv, tail_send, tail_recv):
    row_me = lax.axis_index("row")
    col_me = lax.axis_index("col")
    plane = row_count * col_count
    part = x_hbm.shape[0] // CHUNKS
    h_cols = h_hbm.shape[1]
    do_cols = do_hbm.shape[1]

    def row_peer(k):
        return lax.rem(row_me + k, row_count)

    def col_peer(k):
        return lax.rem(col_me + k, col_count)

    def plane_peers():
        return [{"col": col_peer(dc), "row": row_peer(dr)} for dc in range(col_count) for dr in range(row_count) if dc or dr]

    def start(copies):
        for copy in copies:
            copy.start()

    def wait(copies):
        for copy in copies:
            copy.wait()

    def rows(i):
        return pl.ds(pl.multiple_of(i * part, part), part)

    def load(src, dst, kind, i):
        return pltpu.make_async_copy(src.at[rows(i), :], dst, load_sem.at[kind, i])

    def down_loads(i):
        return [load(h_hbm, mix_buf.at[rows(i), pl.ds(0, h_cols)], 0, i), load(do_hbm, mix_buf.at[rows(i), pl.ds(h_cols, do_cols)], 1, i)]

    def gate_loads(i):
        return [load(x_hbm, x_buf.at[rows(i), :], 2, i), load(dg_hbm, gate_buf.at[rows(i), :], 3, i)]

    def up_loads(i):
        return [load(du_hbm, mix_buf.at[rows(i), :], 4, i)]

    w_copies = [pltpu.make_async_copy(src, dst, w_sem.at[k]) for k, (src, dst) in enumerate(((wd_hbm, w_down), (wg_hbm, w_gate), (wu_hbm, w_up)))]
    stat_copies = [pltpu.make_async_copy(src, dst, small_sem.at[k]) for k, (src, dst) in enumerate(((rg, old_gate_r), (cg, old_gate_c), (ru, old_up_r), (cu, old_up_c), (rd, old_down_r), (cd, old_down_c)))]

    def exchange(kind, buf, own, send_sem, recv_sem, index):
        count, me, peer = (col_count, col_me, col_peer) if kind == "col" else (row_count, row_me, row_peer)
        buf[pl.ds(me, 1)] = own[None]
        for k in range(1, count):
            pltpu.make_async_remote_copy(buf.at[me], buf.at[me], send_sem.at[index], recv_sem.at[index], device_id={kind: peer(k)}, device_id_type=MESH).start()

        def finish():
            for sem in (send_sem, recv_sem):
                pltpu.make_async_copy(buf.at[pl.ds(0, count - 1)], buf.at[pl.ds(0, count - 1)], sem.at[index]).wait()
        return finish

    def sums_out(g_ref, lane_ref, row_buf, col_buf, index):
        def body(s, columns):
            g = g_ref[s, :]
            q = g * g
            lane_ref[s, :] = lane_groups(q)
            return columns + row_groups(q)

        columns = over_rows(g_ref, body, jnp.zeros((SUBLANES, g_ref.shape[1]), F32))
        col_part = jnp.sum(columns, axis=0, keepdims=True) + g_ref.shape[0] * EPS_SQ
        first = exchange("row", col_buf, col_part, col_send, col_recv, index)
        row_part = jnp.sum(lane_ref[...].T, axis=0, keepdims=True) + g_ref.shape[1] * EPS_SQ
        second = exchange("col", row_buf, row_part, row_send, row_recv, index)
        return first, second

    def new_stats(finish, g_ref, row_buf, col_buf, r_old, c_old, r_new, c_new, a_ref, b_ref):
        for part in finish:
            part()
        m_total = g_ref.shape[0] * row_count
        n_total = g_ref.shape[1] * col_count
        beta = beta_ref[...]
        row_sum = tree_sum([row_buf[k] for k in range(col_count)])
        col_sum = tree_sum([col_buf[k] for k in range(row_count)])
        r_val = beta * r_old[...].reshape(1, -1) + (1.0 - beta) * (row_sum / n_total)
        c_val = beta * c_old[...].reshape(1, -1) + (1.0 - beta) * (col_sum / m_total)
        r_new[...] = r_val.reshape(-1)
        c_new[...] = c_val.reshape(-1)
        a_row = 1.0 / jnp.sqrt(r_val)
        b_ref[...] = 1.0 / jnp.sqrt(c_val)
        a_ref[...] = jnp.broadcast_to(a_row, (LANES, a_row.shape[1])).T

        def body(s, total):
            t = g_ref[s, :] * b_ref[...]
            u = lane_groups(t * t) * (a_ref[s, :] * a_ref[s, :])
            return total + row_groups(u)

        return over_rows(g_ref, body, jnp.zeros((SUBLANES, LANES), F32)), lane_groups(r_val)

    def square_sum(w_ref):
        def body(s, total):
            w = w_ref[s, :]
            return total + row_groups(lane_groups(w * w))

        return over_rows(w_ref, body, jnp.zeros((SUBLANES, LANES), F32))

    def matmul(g_ref, loads, act, cot):
        def step(i, carry):
            wait(loads(i))
            product = token_dot(act(rows(i)), cot(rows(i)))
            g_ref[...] = jnp.where(i == 0, 0.0, g_ref[...]) + product
            return carry

        lax.fori_loop(0, CHUNKS, step, 0)

    for i in range(CHUNKS):
        start(down_loads(i))
    for i in range(CHUNKS):
        start(gate_loads(i))
    barrier = pltpu.get_barrier_semaphore()
    for peer in plane_peers():
        pl.semaphore_signal(barrier, inc=1, device_id=peer, device_id_type=MESH)
    matmul(g_down, down_loads, lambda s: mix_buf[s, 0:h_cols], lambda s: mix_buf[s, h_cols : h_cols + do_cols])
    for i in range(CHUNKS):
        start(up_loads(i))
    start(w_copies)
    start(stat_copies)
    pl.semaphore_wait(barrier, plane - 1)
    down_out = sums_out(g_down, a_down, row_down, col_down, 0)
    matmul(g_gate, gate_loads, lambda s: x_buf[s, :], lambda s: gate_buf[s, :])
    gate_out = sums_out(g_gate, a_gate, row_gate, col_gate, 1)
    matmul(g_up, up_loads, lambda s: x_buf[s, :], lambda s: mix_buf[s, :])
    up_out = sums_out(g_up, a_up, row_up, col_up, 2)

    wait(w_copies)
    wait(stat_copies)
    w_sums = [square_sum(w) for w in (w_down, w_gate, w_up)]
    u_down, r_down = new_stats(down_out, g_down, row_down, col_down, old_down_r, old_down_c, rn_down, cn_down, a_down, b_down)
    u_gate, r_gate = new_stats(gate_out, g_gate, row_gate, col_gate, old_gate_r, old_gate_c, rn_gate, cn_gate, a_gate, b_gate)
    u_up, r_up = new_stats(up_out, g_up, row_up, col_up, old_up_r, old_up_c, rn_up, cn_up, a_up, b_up)

    lane = lax.broadcasted_iota(jnp.int32, (1, LANES), 1)
    packed = jnp.zeros((1, LANES), F32)
    for k, value in enumerate(w_sums + [r_down, r_gate, r_up, u_down, u_gate, u_up]):
        packed = jnp.where(lane == k, jnp.sum(jnp.sum(value, axis=0, keepdims=True), axis=1, keepdims=True), packed)
    me = col_me * row_count + row_me
    tail_buf[pl.ds(me, 1)] = packed[None]
    for peer in plane_peers():
        pltpu.make_async_remote_copy(tail_buf.at[me], tail_buf.at[me], tail_send, tail_recv, device_id=peer, device_id_type=MESH).start()
    for sem in (tail_send, tail_recv):
        pltpu.make_async_copy(tail_buf.at[pl.ds(0, plane - 1)], tail_buf.at[pl.ds(0, plane - 1)], sem).wait()
    sums = jnp.sum(tail_buf[...], axis=0)

    def pick(k):
        return jnp.sum(jnp.where(lane == k, sums, 0.0), axis=1, keepdims=True)

    for k, (g_ref, a_ref) in enumerate(((g_down, a_down), (g_gate, a_gate), (g_up, a_up))):
        m_total = g_ref.shape[0] * row_count
        n_total = g_ref.shape[1] * col_count
        r_mean = pick(3 + k) / (m_total * col_count)
        w_rms = jnp.sqrt(pick(k) / (m_total * n_total))
        u_rms = jnp.sqrt(r_mean * pick(6 + k) / (m_total * n_total))
        size = step_ref[...] * jnp.maximum(EPS_SCALE, w_rms)
        scale = size * jnp.sqrt(r_mean) / jnp.maximum(1.0, u_rms / clip_ref[...])
        a_ref[...] = a_ref[...] * scale


PARTS = 4


def apply_kernel(g_gate, g_up, g_down, w_gate, w_up, w_down, a_gate, a_up, a_down, b_gate, b_up, b_down, rn_gate, cn_gate, rn_up, cn_up, rn_down, cn_down,
                 o_gate, o_up, o_down, ro_gate, co_gate, ro_up, co_up, ro_down, co_down, t_gate, t_up, t_down, w_sem, s_sem):
    small = [pltpu.make_async_copy(src, dst, s_sem.at[k]) for k, (src, dst) in enumerate(((rn_gate, ro_gate), (cn_gate, co_gate), (rn_up, ro_up), (cn_up, co_up), (rn_down, ro_down), (cn_down, co_down)))]
    for copy in small:
        copy.start()
    blocks = ((g_down, w_down, a_down, b_down, t_down, o_down), (g_gate, w_gate, a_gate, b_gate, t_gate, o_gate), (g_up, w_up, a_up, b_up, t_up, o_up))

    def out_copy(k, i):
        t, o = blocks[k][4:]
        size = t.shape[0] // PARTS
        s = pl.ds(pl.multiple_of(i * size, size), size)
        return pltpu.make_async_copy(t.at[s, :], o.at[s, :], w_sem.at[k, i])

    for k, (g, w, a, b, t, o) in enumerate(blocks):
        size = g.shape[0] // PARTS
        tile = tile_rows(g)

        def part(i, carry):
            def body(j, inner):
                s = pl.ds(pl.multiple_of(i * size + j * tile, tile), tile)
                a_val = a[s, :]
                for c in range(0, g.shape[1], LANES):
                    ls = pl.ds(c, LANES)
                    t[s, ls] = w[s, ls] - g[s, ls] * (a_val * b[:, ls])
                return inner

            lax.fori_loop(0, size // tile, body, 0)
            out_copy(k, i).start()
            return carry

        lax.fori_loop(0, PARTS, part, 0)
    for k in range(len(blocks)):
        for i in range(PARTS):
            out_copy(k, i).wait()
    for copy in small:
        copy.wait()


def solution(mesh):
    row_count = mesh.shape["row"]
    col_count = mesh.shape["col"]

    def local_program(x_in, h_act, d_gate, d_up, d_out, w_gate, w_up, w_down, r_gate, c_gate, r_up, c_up, r_down, c_down, beta_two, rel_step, clip_thr):
        blocks = (w_gate, w_up, w_down)
        tokens = x_in.shape[0]
        out_shape = [pltpu.VMEM(w.shape, F32) for w in blocks] * 2
        out_shape += [pltpu.VMEM((w.shape[0], LANES), F32) for w in blocks]
        out_shape += [pltpu.VMEM((1, w.shape[1]), F32) for w in blocks]
        stats = [pltpu.VMEM((w.shape[k],), F32) for w in blocks for k in range(2)]
        dma = pltpu.SemaphoreType.DMA
        flops = sum(2 * tokens * w.shape[0] * w.shape[1] for w in blocks)
        mid = pl.pallas_call(
            functools.partial(update_kernel, row_count, col_count),
            out_shape=out_shape + stats,
            in_specs=[HBM_SPEC] * 14 + [SMEM_SPEC] * 3,
            out_specs=[VMEM_SPEC] * 18,
            scratch_shapes=[
                pltpu.VMEM(x_in.shape, BF16),
                pltpu.VMEM(d_gate.shape, BF16),
                pltpu.VMEM((tokens, max(d_up.shape[1], h_act.shape[1] + d_out.shape[1])), BF16),
                *[pltpu.VMEM((col_count, 1, w.shape[0]), F32) for w in blocks],
                *[pltpu.VMEM((row_count, 1, w.shape[1]), F32) for w in blocks],
                pltpu.VMEM((row_count * col_count, 1, LANES), F32),
                *[pltpu.VMEM((w.shape[k],), F32) for w in blocks for k in range(2)],
                dma((5, CHUNKS)), dma((3,)), dma((6,)), dma((3,)), dma((3,)), dma((3,)), dma((3,)), dma, dma,
            ],
            compiler_params=pltpu.CompilerParams(collective_id=0, has_side_effects=True, vmem_limit_bytes=VMEM_A),
            cost_estimate=pl.CostEstimate(flops=flops, bytes_accessed=60_000_000, transcendentals=0),
            name="grad_and_stats",
        )(x_in, h_act, d_gate, d_up, d_out, w_gate, w_up, w_down, r_gate, c_gate, r_up, c_up, r_down, c_down, beta_two, rel_step, clip_thr)
        out = pl.pallas_call(
            apply_kernel,
            out_shape=[jax.ShapeDtypeStruct(w.shape, F32) for w in blocks] + [jax.ShapeDtypeStruct((w.shape[k],), F32) for w in blocks for k in range(2)],
            in_specs=[VMEM_SPEC] * 18,
            out_specs=[HBM_SPEC] * 9,
            scratch_shapes=[pltpu.VMEM(w.shape, F32) for w in blocks] + [dma((3, PARTS)), dma((6,))],
            compiler_params=pltpu.CompilerParams(vmem_limit_bytes=VMEM_B),
            cost_estimate=pl.CostEstimate(flops=10_000_000, bytes_accessed=10_000_000, transcendentals=0),
            name="apply_update",
        )(*mid)
        return tuple(out)

    act_spec = P(None, "row")
    cot_spec = P(None, "col")
    w_spec = P("row", "col")
    r_spec = P("row")
    c_spec = P("col")
    s_spec = P()
    return jax.shard_map(local_program, mesh=mesh, in_specs=(act_spec, act_spec, cot_spec, cot_spec, cot_spec, w_spec, w_spec, w_spec, r_spec, c_spec, r_spec, c_spec, r_spec, c_spec, s_spec, s_spec, s_spec), out_specs=(w_spec, w_spec, w_spec, r_spec, c_spec, r_spec, c_spec, r_spec, c_spec), check_vma=False)
```

```python
import functools

import jax
import jax.numpy as jnp
from jax import lax
from jax.experimental import pallas as pl
from jax.experimental.pallas import tpu as pltpu
from jax.sharding import PartitionSpec as P

F32 = jnp.float32
BF16 = jnp.bfloat16
MESH = pl.DeviceIdType.MESH
EPS_SQ = 1e-30
EPS_SCALE = 1e-3
LANES = 128
SUBLANES = 8
DOWN_CHUNKS = 4
GATE_CHUNKS = 2
UP_CHUNKS = 2
CONTRACT_TOKENS = (((0,), (0,)), ((), ()))
VMEM_SPEC = pl.BlockSpec(memory_space=pltpu.VMEM)
HBM_SPEC = pl.BlockSpec(memory_space=pltpu.HBM)
SMEM_SPEC = pl.BlockSpec(memory_space=pltpu.SMEM)
VMEM_A = 44 * 2**20
VMEM_B = 14 * 2**20


def token_dot(act, cot):
    return lax.dot_general(act, cot, CONTRACT_TOKENS, preferred_element_type=F32)


def tree_sum(parts):
    while len(parts) > 1:
        parts = [sum(parts[k + 1 : k + 2], parts[k]) for k in range(0, len(parts), 2)]
    return parts[0]


def lane_groups(value):
    return tree_sum([value[:, k : k + LANES] for k in range(0, value.shape[1], LANES)])


def row_groups(value):
    return tree_sum([value[k : k + SUBLANES] for k in range(0, value.shape[0], SUBLANES)])


def tile_rows(ref):
    return 64 if ref.shape[1] > 1024 else 128


def over_rows(ref, body, init):
    size = tile_rows(ref)
    return lax.fori_loop(0, ref.shape[0] // size, lambda i, carry: body(pl.ds(pl.multiple_of(i * size, size), size), carry), init)


def update_kernel(row_count, col_count, x_hbm, h_hbm, dg_hbm, du_hbm, do_hbm, wg_hbm, wu_hbm, wd_hbm, rg, cg, ru, cu, rd, cd, beta_ref, step_ref, clip_ref,
                  g_gate, g_up, g_down, w_gate, w_up, w_down, a_gate, a_up, a_down, b_gate, b_up, b_down, rn_gate, cn_gate, rn_up, cn_up, rn_down, cn_down,
                  x_buf, gate_buf, mix_buf, row_gate, row_up, row_down, col_gate, col_up, col_down, tail_buf,
                  old_gate_r, old_gate_c, old_up_r, old_up_c, old_down_r, old_down_c, load_sem, w_sem, small_sem, row_send, row_recv, col_send, col_recv, tail_send, tail_recv):
    row_me = lax.axis_index("row")
    col_me = lax.axis_index("col")
    plane = row_count * col_count
    tokens = x_hbm.shape[0]
    h_cols = h_hbm.shape[1]
    do_cols = do_hbm.shape[1]

    def row_peer(k):
        return lax.rem(row_me + k, row_count)

    def col_peer(k):
        return lax.rem(col_me + k, col_count)

    def plane_peers():
        return [{"col": col_peer(dc), "row": row_peer(dr)} for dc in range(col_count) for dr in range(row_count) if dc or dr]

    def start(copies):
        for copy in copies:
            copy.start()

    def wait(copies):
        for copy in copies:
            copy.wait()

    def rows(i, count):
        return pl.ds(pl.multiple_of(i * (tokens // count), tokens // count), tokens // count)

    def load(src, dst, s, kind, i):
        return pltpu.make_async_copy(src.at[s, :], dst, load_sem.at[kind, i])

    def down_loads(i):
        s = rows(i, DOWN_CHUNKS)
        return [load(h_hbm, mix_buf.at[s, pl.ds(0, h_cols)], s, 0, i), load(do_hbm, mix_buf.at[s, pl.ds(h_cols, do_cols)], s, 1, i)]

    def gate_loads(i):
        s = rows(i, GATE_CHUNKS)
        return [load(x_hbm, x_buf.at[s, :], s, 2, i), load(dg_hbm, gate_buf.at[s, :], s, 3, i)]

    def up_loads(i):
        s = rows(i, UP_CHUNKS)
        return [load(du_hbm, mix_buf.at[s, :], s, 4, i)]

    w_copies = [pltpu.make_async_copy(src, dst, w_sem.at[k]) for k, (src, dst) in enumerate(((wd_hbm, w_down), (wg_hbm, w_gate), (wu_hbm, w_up)))]
    stat_copies = [pltpu.make_async_copy(src, dst, small_sem.at[k]) for k, (src, dst) in enumerate(((rg, old_gate_r), (cg, old_gate_c), (ru, old_up_r), (cu, old_up_c), (rd, old_down_r), (cd, old_down_c)))]

    def exchange(kind, buf, own, send_sem, recv_sem, index):
        count, me, peer = (col_count, col_me, col_peer) if kind == "col" else (row_count, row_me, row_peer)
        buf[pl.ds(me, 1)] = own[None]
        for k in range(1, count):
            pltpu.make_async_remote_copy(buf.at[me], buf.at[me], send_sem.at[index], recv_sem.at[index], device_id={kind: peer(k)}, device_id_type=MESH).start()

        def finish():
            for sem in (send_sem, recv_sem):
                pltpu.make_async_copy(buf.at[pl.ds(0, count - 1)], buf.at[pl.ds(0, count - 1)], sem.at[index]).wait()
        return finish

    def block_sums(g_ref, lane_ref, s, columns):
        g = g_ref[s, :]
        q = g * g
        lane_ref[s, :] = lane_groups(q)
        return columns + row_groups(q)

    def no_columns(g_ref):
        return jnp.zeros((SUBLANES, g_ref.shape[1]), F32)

    def send_sums(columns, g_ref, lane_ref, row_buf, col_buf, index):
        col_part = jnp.sum(columns, axis=0, keepdims=True) + g_ref.shape[0] * EPS_SQ
        first = exchange("row", col_buf, col_part, col_send, col_recv, index)
        row_part = jnp.sum(lane_ref[...].T, axis=0, keepdims=True) + g_ref.shape[1] * EPS_SQ
        second = exchange("col", row_buf, row_part, row_send, row_recv, index)
        return first, second

    def new_stats(finish, g_ref, row_buf, col_buf, r_old, c_old, r_new, c_new, a_ref, b_ref):
        for part in finish:
            part()
        m_total = g_ref.shape[0] * row_count
        n_total = g_ref.shape[1] * col_count
        beta = beta_ref[...]
        row_sum = tree_sum([row_buf[k] for k in range(col_count)])
        col_sum = tree_sum([col_buf[k] for k in range(row_count)])
        r_val = beta * r_old[...].reshape(1, -1) + (1.0 - beta) * (row_sum / n_total)
        c_val = beta * c_old[...].reshape(1, -1) + (1.0 - beta) * (col_sum / m_total)
        r_new[...] = r_val.reshape(-1)
        c_new[...] = c_val.reshape(-1)
        a_row = 1.0 / jnp.sqrt(r_val)
        b_ref[...] = 1.0 / jnp.sqrt(c_val)
        a_ref[...] = jnp.broadcast_to(a_row, (LANES, a_row.shape[1])).T

        def body(s, total):
            t = g_ref[s, :] * b_ref[...]
            u = lane_groups(t * t) * (a_ref[s, :] * a_ref[s, :])
            return total + row_groups(u)

        return over_rows(g_ref, body, jnp.zeros((SUBLANES, LANES), F32)), lane_groups(r_val)

    def square_sum(w_ref):
        def body(s, total):
            w = w_ref[s, :]
            return total + row_groups(lane_groups(w * w))

        return over_rows(w_ref, body, jnp.zeros((SUBLANES, LANES), F32))

    def matmul(g_ref, count, loads, act, cot, beside, init):
        def step(i, carry):
            wait(loads(i))
            carry = beside(i, carry)
            product = token_dot(act(rows(i, count)), cot(rows(i, count)))
            g_ref[...] = jnp.where(i == 0, 0.0, g_ref[...]) + product
            return carry

        return lax.fori_loop(0, count, step, init)

    for i in range(DOWN_CHUNKS):
        start(down_loads(i))
    for i in range(GATE_CHUNKS):
        start(gate_loads(i))
    barrier = pltpu.get_barrier_semaphore()
    for peer in plane_peers():
        pl.semaphore_signal(barrier, inc=1, device_id=peer, device_id_type=MESH)
    matmul(g_down, DOWN_CHUNKS, down_loads, lambda s: mix_buf[s, 0:h_cols], lambda s: mix_buf[s, h_cols : h_cols + do_cols], lambda i, c: c, 0)
    for i in range(UP_CHUNKS):
        start(up_loads(i))
    start(w_copies)
    start(stat_copies)
    pl.semaphore_wait(barrier, plane - 1)

    def down_sums(i, columns):
        size = g_down.shape[0] // GATE_CHUNKS
        return block_sums(g_down, a_down, pl.ds(pl.multiple_of(i * size, size), size), columns)

    columns = matmul(g_gate, GATE_CHUNKS, gate_loads, lambda s: x_buf[s, :], lambda s: gate_buf[s, :], down_sums, no_columns(g_down))
    down_out = send_sums(columns, g_down, a_down, row_down, col_down, 0)
    columns = over_rows(g_gate, lambda s, c: block_sums(g_gate, a_gate, s, c), no_columns(g_gate))
    gate_out = send_sums(columns, g_gate, a_gate, row_gate, col_gate, 1)

    matmul(g_up, UP_CHUNKS, up_loads, lambda s: x_buf[s, :], lambda s: mix_buf[s, :], lambda i, c: c, 0)
    columns = over_rows(g_up, lambda s, c: block_sums(g_up, a_up, s, c), no_columns(g_up))
    up_out = send_sums(columns, g_up, a_up, row_up, col_up, 2)

    wait(w_copies)
    wait(stat_copies)
    w_sums = [square_sum(w) for w in (w_down, w_gate, w_up)]
    u_down, r_down = new_stats(down_out, g_down, row_down, col_down, old_down_r, old_down_c, rn_down, cn_down, a_down, b_down)
    u_gate, r_gate = new_stats(gate_out, g_gate, row_gate, col_gate, old_gate_r, old_gate_c, rn_gate, cn_gate, a_gate, b_gate)
    u_up, r_up = new_stats(up_out, g_up, row_up, col_up, old_up_r, old_up_c, rn_up, cn_up, a_up, b_up)

    lane = lax.broadcasted_iota(jnp.int32, (1, LANES), 1)
    packed = jnp.zeros((1, LANES), F32)
    for k, value in enumerate(w_sums + [r_down, r_gate, r_up, u_down, u_gate, u_up]):
        packed = jnp.where(lane == k, jnp.sum(jnp.sum(value, axis=0, keepdims=True), axis=1, keepdims=True), packed)
    me = col_me * row_count + row_me
    tail_buf[pl.ds(me, 1)] = packed[None]
    for peer in plane_peers():
        pltpu.make_async_remote_copy(tail_buf.at[me], tail_buf.at[me], tail_send, tail_recv, device_id=peer, device_id_type=MESH).start()
    for sem in (tail_send, tail_recv):
        pltpu.make_async_copy(tail_buf.at[pl.ds(0, plane - 1)], tail_buf.at[pl.ds(0, plane - 1)], sem).wait()
    sums = jnp.sum(tail_buf[...], axis=0)

    def pick(k):
        return jnp.sum(jnp.where(lane == k, sums, 0.0), axis=1, keepdims=True)

    for k, (g_ref, a_ref) in enumerate(((g_down, a_down), (g_gate, a_gate), (g_up, a_up))):
        m_total = g_ref.shape[0] * row_count
        n_total = g_ref.shape[1] * col_count
        r_mean = pick(3 + k) / (m_total * col_count)
        w_rms = jnp.sqrt(pick(k) / (m_total * n_total))
        u_rms = jnp.sqrt(r_mean * pick(6 + k) / (m_total * n_total))
        size = step_ref[...] * jnp.maximum(EPS_SCALE, w_rms)
        scale = size * jnp.sqrt(r_mean) / jnp.maximum(1.0, u_rms / clip_ref[...])
        a_ref[...] = a_ref[...] * scale


PARTS = 4


def apply_kernel(g_gate, g_up, g_down, w_gate, w_up, w_down, a_gate, a_up, a_down, b_gate, b_up, b_down, rn_gate, cn_gate, rn_up, cn_up, rn_down, cn_down,
                 o_gate, o_up, o_down, ro_gate, co_gate, ro_up, co_up, ro_down, co_down, t_gate, t_up, t_down, w_sem, s_sem):
    small = [pltpu.make_async_copy(src, dst, s_sem.at[k]) for k, (src, dst) in enumerate(((rn_gate, ro_gate), (cn_gate, co_gate), (rn_up, ro_up), (cn_up, co_up), (rn_down, ro_down), (cn_down, co_down)))]
    for copy in small:
        copy.start()
    blocks = ((g_down, w_down, a_down, b_down, t_down, o_down), (g_gate, w_gate, a_gate, b_gate, t_gate, o_gate), (g_up, w_up, a_up, b_up, t_up, o_up))

    def out_copy(k, i):
        t, o = blocks[k][4:]
        size = t.shape[0] // PARTS
        s = pl.ds(pl.multiple_of(i * size, size), size)
        return pltpu.make_async_copy(t.at[s, :], o.at[s, :], w_sem.at[k, i])

    for k, (g, w, a, b, t, o) in enumerate(blocks):
        size = g.shape[0] // PARTS
        tile = min(tile_rows(g) // 2, size)

        def part(i, carry):
            def body(j, inner):
                s = pl.ds(pl.multiple_of(i * size + j * tile, tile), tile)
                a_val = a[s, :]
                for c in range(0, g.shape[1], LANES):
                    ls = pl.ds(c, LANES)
                    t[s, ls] = w[s, ls] - g[s, ls] * (a_val * b[:, ls])
                return inner

            lax.fori_loop(0, size // tile, body, 0)
            out_copy(k, i).start()
            return carry

        lax.fori_loop(0, PARTS, part, 0)
    for k in range(len(blocks)):
        for i in range(PARTS):
            out_copy(k, i).wait()
    for copy in small:
        copy.wait()


def solution(mesh):
    row_count = mesh.shape["row"]
    col_count = mesh.shape["col"]

    def local_program(x_in, h_act, d_gate, d_up, d_out, w_gate, w_up, w_down, r_gate, c_gate, r_up, c_up, r_down, c_down, beta_two, rel_step, clip_thr):
        blocks = (w_gate, w_up, w_down)
        tokens = x_in.shape[0]
        out_shape = [pltpu.VMEM(w.shape, F32) for w in blocks] * 2
        out_shape += [pltpu.VMEM((w.shape[0], LANES), F32) for w in blocks]
        out_shape += [pltpu.VMEM((1, w.shape[1]), F32) for w in blocks]
        stats = [pltpu.VMEM((w.shape[k],), F32) for w in blocks for k in range(2)]
        dma = pltpu.SemaphoreType.DMA
        flops = sum(2 * tokens * w.shape[0] * w.shape[1] for w in blocks)
        mid = pl.pallas_call(
            functools.partial(update_kernel, row_count, col_count),
            out_shape=out_shape + stats,
            in_specs=[HBM_SPEC] * 14 + [SMEM_SPEC] * 3,
            out_specs=[VMEM_SPEC] * 18,
            scratch_shapes=[
                pltpu.VMEM(x_in.shape, BF16),
                pltpu.VMEM(d_gate.shape, BF16),
                pltpu.VMEM((tokens, max(d_up.shape[1], h_act.shape[1] + d_out.shape[1])), BF16),
                *[pltpu.VMEM((col_count, 1, w.shape[0]), F32) for w in blocks],
                *[pltpu.VMEM((row_count, 1, w.shape[1]), F32) for w in blocks],
                pltpu.VMEM((row_count * col_count, 1, LANES), F32),
                *[pltpu.VMEM((w.shape[k],), F32) for w in blocks for k in range(2)],
                dma((5, 4)), dma((3,)), dma((6,)), dma((3,)), dma((3,)), dma((3,)), dma((3,)), dma, dma,
            ],
            compiler_params=pltpu.CompilerParams(collective_id=0, has_side_effects=True, vmem_limit_bytes=VMEM_A),
            cost_estimate=pl.CostEstimate(flops=flops, bytes_accessed=60_000_000, transcendentals=0),
            name="grad_and_stats",
        )(x_in, h_act, d_gate, d_up, d_out, w_gate, w_up, w_down, r_gate, c_gate, r_up, c_up, r_down, c_down, beta_two, rel_step, clip_thr)
        out = pl.pallas_call(
            apply_kernel,
            out_shape=[jax.ShapeDtypeStruct(w.shape, F32) for w in blocks] + [jax.ShapeDtypeStruct((w.shape[k],), F32) for w in blocks for k in range(2)],
            in_specs=[VMEM_SPEC] * 18,
            out_specs=[HBM_SPEC] * 9,
            scratch_shapes=[pltpu.VMEM(w.shape, F32) for w in blocks] + [dma((3, PARTS)), dma((6,))],
            compiler_params=pltpu.CompilerParams(vmem_limit_bytes=VMEM_B),
            cost_estimate=pl.CostEstimate(flops=10_000_000, bytes_accessed=10_000_000, transcendentals=0),
            name="apply_update",
        )(*mid)
        return tuple(out)

    act_spec = P(None, "row")
    cot_spec = P(None, "col")
    w_spec = P("row", "col")
    r_spec = P("row")
    c_spec = P("col")
    s_spec = P()
    return jax.shard_map(local_program, mesh=mesh, in_specs=(act_spec, act_spec, cot_spec, cot_spec, cot_spec, w_spec, w_spec, w_spec, r_spec, c_spec, r_spec, c_spec, r_spec, c_spec, s_spec, s_spec, s_spec), out_specs=(w_spec, w_spec, w_spec, r_spec, c_spec, r_spec, c_spec, r_spec, c_spec), check_vma=False)
```

```python
import functools

import jax
import jax.numpy as jnp
from jax import lax
from jax.experimental import pallas as pl
from jax.experimental.pallas import tpu as pltpu
from jax.sharding import PartitionSpec as P

F32 = jnp.float32
BF16 = jnp.bfloat16
MESH = pl.DeviceIdType.MESH
EPS_SQ = 1e-30
EPS_SCALE = 1e-3
LANES = 128
SUBLANES = 8
DOWN_CHUNKS = 4
GATE_CHUNKS = 2
UP_CHUNKS = 2
CONTRACT_TOKENS = (((0,), (0,)), ((), ()))
VMEM_SPEC = pl.BlockSpec(memory_space=pltpu.VMEM)
HBM_SPEC = pl.BlockSpec(memory_space=pltpu.HBM)
SMEM_SPEC = pl.BlockSpec(memory_space=pltpu.SMEM)
VMEM_A = 44 * 2**20
VMEM_B = 14 * 2**20


def token_dot(act, cot):
    return lax.dot_general(act, cot, CONTRACT_TOKENS, preferred_element_type=F32)


def tree_sum(parts):
    while len(parts) > 1:
        parts = [sum(parts[k + 1 : k + 2], parts[k]) for k in range(0, len(parts), 2)]
    return parts[0]


def lane_groups(value):
    return tree_sum([value[:, k : k + LANES] for k in range(0, value.shape[1], LANES)])


def row_groups(value):
    return tree_sum([value[k : k + SUBLANES] for k in range(0, value.shape[0], SUBLANES)])


def tile_rows(ref):
    return 64 if ref.shape[1] > 1024 else 128


def over_rows(ref, body, init):
    size = tile_rows(ref)
    return lax.fori_loop(0, ref.shape[0] // size, lambda i, carry: body(pl.ds(pl.multiple_of(i * size, size), size), carry), init)


def update_kernel(row_count, col_count, x_hbm, h_hbm, dg_hbm, du_hbm, do_hbm, wg_hbm, wu_hbm, wd_hbm, rg, cg, ru, cu, rd, cd, beta_ref, step_ref, clip_ref,
                  g_gate, g_up, g_down, w_gate, w_up, w_down, a_gate, a_up, a_down, b_gate, b_up, b_down, rn_gate, cn_gate, rn_up, cn_up, rn_down, cn_down,
                  x_buf, gate_buf, mix_buf, row_gate, row_up, row_down, col_gate, col_up, col_down, tail_buf,
                  old_gate_r, old_gate_c, old_up_r, old_up_c, old_down_r, old_down_c, load_sem, w_sem, small_sem, row_send, row_recv, col_send, col_recv, tail_send, tail_recv):
    row_me = lax.axis_index("row")
    col_me = lax.axis_index("col")
    plane = row_count * col_count
    tokens = x_hbm.shape[0]
    h_cols = h_hbm.shape[1]
    do_cols = do_hbm.shape[1]

    def row_peer(k):
        return lax.rem(row_me + k, row_count)

    def col_peer(k):
        return lax.rem(col_me + k, col_count)

    def farthest_first(count):
        return sorted(range(1, count), key=lambda k: -min(k, count - k))

    def plane_peers():
        offsets = [(dc, dr) for dc in range(col_count) for dr in range(row_count) if dc or dr]
        offsets.sort(key=lambda o: -min(o[0], col_count - o[0]) - min(o[1], row_count - o[1]) / 2)
        return [{"col": col_peer(dc), "row": row_peer(dr)} for dc, dr in offsets]

    def start(copies):
        for copy in copies:
            copy.start()

    def wait(copies):
        for copy in copies:
            copy.wait()

    def rows(i, count):
        return pl.ds(pl.multiple_of(i * (tokens // count), tokens // count), tokens // count)

    def load(src, dst, s, kind, i):
        return pltpu.make_async_copy(src.at[s, :], dst, load_sem.at[kind, i])

    def down_loads(i):
        s = rows(i, DOWN_CHUNKS)
        return [load(h_hbm, mix_buf.at[s, pl.ds(0, h_cols)], s, 0, i), load(do_hbm, mix_buf.at[s, pl.ds(h_cols, do_cols)], s, 1, i)]

    def gate_loads(i):
        s = rows(i, GATE_CHUNKS)
        return [load(x_hbm, x_buf.at[s, :], s, 2, i), load(dg_hbm, gate_buf.at[s, :], s, 3, i)]

    def up_loads(i):
        s = rows(i, UP_CHUNKS)
        return [load(du_hbm, mix_buf.at[s, :], s, 4, i)]

    w_copies = [pltpu.make_async_copy(src, dst, w_sem.at[k]) for k, (src, dst) in enumerate(((wd_hbm, w_down), (wg_hbm, w_gate), (wu_hbm, w_up)))]
    stat_copies = [pltpu.make_async_copy(src, dst, small_sem.at[k]) for k, (src, dst) in enumerate(((rg, old_gate_r), (cg, old_gate_c), (ru, old_up_r), (cu, old_up_c), (rd, old_down_r), (cd, old_down_c)))]

    def exchange(kind, buf, own, send_sem, recv_sem, index):
        count, me, peer = (col_count, col_me, col_peer) if kind == "col" else (row_count, row_me, row_peer)
        buf[pl.ds(me, 1)] = own[None]
        for k in farthest_first(count):
            pltpu.make_async_remote_copy(buf.at[me], buf.at[me], send_sem.at[index], recv_sem.at[index], device_id={kind: peer(k)}, device_id_type=MESH).start()

        def finish():
            for sem in (send_sem, recv_sem):
                pltpu.make_async_copy(buf.at[pl.ds(0, count - 1)], buf.at[pl.ds(0, count - 1)], sem.at[index]).wait()
        return finish

    def block_sums(g_ref, lane_ref, s, columns):
        g = g_ref[s, :]
        q = g * g
        lane_ref[s, :] = lane_groups(q)
        return columns + row_groups(q)

    def no_columns(g_ref):
        return jnp.zeros((SUBLANES, g_ref.shape[1]), F32)

    def send_sums(columns, g_ref, lane_ref, row_buf, col_buf, index):
        col_part = jnp.sum(columns, axis=0, keepdims=True) + g_ref.shape[0] * EPS_SQ
        row_part = jnp.sum(lane_ref[...].T, axis=0, keepdims=True) + g_ref.shape[1] * EPS_SQ
        first = exchange("row", col_buf, col_part, col_send, col_recv, index)
        second = exchange("col", row_buf, row_part, row_send, row_recv, index)
        return first, second

    def new_stats(finish, g_ref, row_buf, col_buf, r_old, c_old, r_new, c_new, a_ref, b_ref):
        finish_columns, finish_rows = finish
        finish_rows()
        m_total = g_ref.shape[0] * row_count
        n_total = g_ref.shape[1] * col_count
        beta = beta_ref[...]
        row_sum = tree_sum([row_buf[k] for k in range(col_count)])
        r_val = beta * r_old[...].reshape(1, -1) + (1.0 - beta) * (row_sum / n_total)
        r_new[...] = r_val.reshape(-1)
        a_row = 1.0 / jnp.sqrt(r_val)
        a_ref[...] = jnp.broadcast_to(a_row, (LANES, a_row.shape[1])).T
        finish_columns()
        col_sum = tree_sum([col_buf[k] for k in range(row_count)])
        c_val = beta * c_old[...].reshape(1, -1) + (1.0 - beta) * (col_sum / m_total)
        c_new[...] = c_val.reshape(-1)
        b_ref[...] = 1.0 / jnp.sqrt(c_val)

        def body(s, total):
            t = g_ref[s, :] * b_ref[...]
            u = lane_groups(t * t) * (a_ref[s, :] * a_ref[s, :])
            return total + row_groups(u)

        return over_rows(g_ref, body, jnp.zeros((SUBLANES, LANES), F32)), lane_groups(r_val)

    def square_sum(w_ref):
        def body(s, total):
            w = w_ref[s, :]
            return total + row_groups(lane_groups(w * w))

        return over_rows(w_ref, body, jnp.zeros((SUBLANES, LANES), F32))

    def matmul(g_ref, count, loads, act, cot, beside, init):
        def step(i, carry):
            wait(loads(i))
            carry = beside(i, carry)
            product = token_dot(act(rows(i, count)), cot(rows(i, count)))
            g_ref[...] = jnp.where(i == 0, 0.0, g_ref[...]) + product
            return carry

        return lax.fori_loop(0, count, step, init)

    for i in range(DOWN_CHUNKS):
        start(down_loads(i))
    for i in range(GATE_CHUNKS):
        start(gate_loads(i))
    barrier = pltpu.get_barrier_semaphore()
    for peer in plane_peers():
        pl.semaphore_signal(barrier, inc=1, device_id=peer, device_id_type=MESH)
    matmul(g_down, DOWN_CHUNKS, down_loads, lambda s: mix_buf[s, 0:h_cols], lambda s: mix_buf[s, h_cols : h_cols + do_cols], lambda i, c: c, 0)
    for i in range(UP_CHUNKS):
        start(up_loads(i))
    start(w_copies)
    start(stat_copies)
    pl.semaphore_wait(barrier, plane - 1)

    def down_sums(i, columns):
        size = g_down.shape[0] // GATE_CHUNKS
        return block_sums(g_down, a_down, pl.ds(pl.multiple_of(i * size, size), size), columns)

    columns = matmul(g_gate, GATE_CHUNKS, gate_loads, lambda s: x_buf[s, :], lambda s: gate_buf[s, :], down_sums, no_columns(g_down))
    down_out = send_sums(columns, g_down, a_down, row_down, col_down, 0)
    columns = over_rows(g_gate, lambda s, c: block_sums(g_gate, a_gate, s, c), no_columns(g_gate))
    gate_out = send_sums(columns, g_gate, a_gate, row_gate, col_gate, 1)

    matmul(g_up, UP_CHUNKS, up_loads, lambda s: x_buf[s, :], lambda s: mix_buf[s, :], lambda i, c: c, 0)
    columns = over_rows(g_up, lambda s, c: block_sums(g_up, a_up, s, c), no_columns(g_up))
    up_out = send_sums(columns, g_up, a_up, row_up, col_up, 2)

    wait(w_copies)
    wait(stat_copies)
    w_sums = [square_sum(w) for w in (w_down, w_gate, w_up)]
    u_down, r_down = new_stats(down_out, g_down, row_down, col_down, old_down_r, old_down_c, rn_down, cn_down, a_down, b_down)
    u_gate, r_gate = new_stats(gate_out, g_gate, row_gate, col_gate, old_gate_r, old_gate_c, rn_gate, cn_gate, a_gate, b_gate)
    u_up, r_up = new_stats(up_out, g_up, row_up, col_up, old_up_r, old_up_c, rn_up, cn_up, a_up, b_up)

    lane = lax.broadcasted_iota(jnp.int32, (1, LANES), 1)
    packed = jnp.zeros((1, LANES), F32)
    for k, value in enumerate(w_sums + [r_down, r_gate, r_up, u_down, u_gate, u_up]):
        packed = jnp.where(lane == k, jnp.sum(jnp.sum(value, axis=0, keepdims=True), axis=1, keepdims=True), packed)
    me = col_me * row_count + row_me
    tail_buf[pl.ds(me, 1)] = packed[None]
    for peer in plane_peers():
        pltpu.make_async_remote_copy(tail_buf.at[me], tail_buf.at[me], tail_send, tail_recv, device_id=peer, device_id_type=MESH).start()
    for sem in (tail_send, tail_recv):
        pltpu.make_async_copy(tail_buf.at[pl.ds(0, plane - 1)], tail_buf.at[pl.ds(0, plane - 1)], sem).wait()
    sums = jnp.sum(tail_buf[...], axis=0)

    def pick(k):
        return jnp.sum(jnp.where(lane == k, sums, 0.0), axis=1, keepdims=True)

    for k, (g_ref, a_ref) in enumerate(((g_down, a_down), (g_gate, a_gate), (g_up, a_up))):
        m_total = g_ref.shape[0] * row_count
        n_total = g_ref.shape[1] * col_count
        r_mean = pick(3 + k) / (m_total * col_count)
        w_rms = jnp.sqrt(pick(k) / (m_total * n_total))
        u_rms = jnp.sqrt(r_mean * pick(6 + k) / (m_total * n_total))
        size = step_ref[...] * jnp.maximum(EPS_SCALE, w_rms)
        scale = size * jnp.sqrt(r_mean) / jnp.maximum(1.0, u_rms / clip_ref[...])
        a_ref[...] = a_ref[...] * scale


PARTS = 4


def apply_kernel(g_gate, g_up, g_down, w_gate, w_up, w_down, a_gate, a_up, a_down, b_gate, b_up, b_down, rn_gate, cn_gate, rn_up, cn_up, rn_down, cn_down,
                 o_gate, o_up, o_down, ro_gate, co_gate, ro_up, co_up, ro_down, co_down, t_gate, t_up, t_down, w_sem, s_sem):
    small = [pltpu.make_async_copy(src, dst, s_sem.at[k]) for k, (src, dst) in enumerate(((rn_gate, ro_gate), (cn_gate, co_gate), (rn_up, ro_up), (cn_up, co_up), (rn_down, ro_down), (cn_down, co_down)))]
    for copy in small:
        copy.start()
    blocks = ((g_down, w_down, a_down, b_down, t_down, o_down), (g_gate, w_gate, a_gate, b_gate, t_gate, o_gate), (g_up, w_up, a_up, b_up, t_up, o_up))

    def out_copy(k, i):
        t, o = blocks[k][4:]
        size = t.shape[0] // PARTS
        s = pl.ds(pl.multiple_of(i * size, size), size)
        return pltpu.make_async_copy(t.at[s, :], o.at[s, :], w_sem.at[k, i])

    for k, (g, w, a, b, t, o) in enumerate(blocks):
        size = g.shape[0] // PARTS
        tile = min(tile_rows(g) // 2, size)

        def part(i, carry):
            def body(j, inner):
                s = pl.ds(pl.multiple_of(i * size + j * tile, tile), tile)
                a_val = a[s, :]
                for c in range(0, g.shape[1], LANES):
                    ls = pl.ds(c, LANES)
                    t[s, ls] = w[s, ls] - g[s, ls] * (a_val * b[:, ls])
                return inner

            lax.fori_loop(0, size // tile, body, 0)
            out_copy(k, i).start()
            return carry

        lax.fori_loop(0, PARTS, part, 0)
    for k in range(len(blocks)):
        for i in range(PARTS):
            out_copy(k, i).wait()
    for copy in small:
        copy.wait()


def solution(mesh):
    row_count = mesh.shape["row"]
    col_count = mesh.shape["col"]

    def local_program(x_in, h_act, d_gate, d_up, d_out, w_gate, w_up, w_down, r_gate, c_gate, r_up, c_up, r_down, c_down, beta_two, rel_step, clip_thr):
        blocks = (w_gate, w_up, w_down)
        tokens = x_in.shape[0]
        out_shape = [pltpu.VMEM(w.shape, F32) for w in blocks] * 2
        out_shape += [pltpu.VMEM((w.shape[0], LANES), F32) for w in blocks]
        out_shape += [pltpu.VMEM((1, w.shape[1]), F32) for w in blocks]
        stats = [pltpu.VMEM((w.shape[k],), F32) for w in blocks for k in range(2)]
        dma = pltpu.SemaphoreType.DMA
        flops = sum(2 * tokens * w.shape[0] * w.shape[1] for w in blocks)
        mid = pl.pallas_call(
            functools.partial(update_kernel, row_count, col_count),
            out_shape=out_shape + stats,
            in_specs=[HBM_SPEC] * 14 + [SMEM_SPEC] * 3,
            out_specs=[VMEM_SPEC] * 18,
            scratch_shapes=[
                pltpu.VMEM(x_in.shape, BF16),
                pltpu.VMEM(d_gate.shape, BF16),
                pltpu.VMEM((tokens, max(d_up.shape[1], h_act.shape[1] + d_out.shape[1])), BF16),
                *[pltpu.VMEM((col_count, 1, w.shape[0]), F32) for w in blocks],
                *[pltpu.VMEM((row_count, 1, w.shape[1]), F32) for w in blocks],
                pltpu.VMEM((row_count * col_count, 1, LANES), F32),
                *[pltpu.VMEM((w.shape[k],), F32) for w in blocks for k in range(2)],
                dma((5, 4)), dma((3,)), dma((6,)), dma((3,)), dma((3,)), dma((3,)), dma((3,)), dma, dma,
            ],
            compiler_params=pltpu.CompilerParams(collective_id=0, has_side_effects=True, vmem_limit_bytes=VMEM_A),
            cost_estimate=pl.CostEstimate(flops=flops, bytes_accessed=60_000_000, transcendentals=0),
            name="grad_and_stats",
        )(x_in, h_act, d_gate, d_up, d_out, w_gate, w_up, w_down, r_gate, c_gate, r_up, c_up, r_down, c_down, beta_two, rel_step, clip_thr)
        out = pl.pallas_call(
            apply_kernel,
            out_shape=[jax.ShapeDtypeStruct(w.shape, F32) for w in blocks] + [jax.ShapeDtypeStruct((w.shape[k],), F32) for w in blocks for k in range(2)],
            in_specs=[VMEM_SPEC] * 18,
            out_specs=[HBM_SPEC] * 9,
            scratch_shapes=[pltpu.VMEM(w.shape, F32) for w in blocks] + [dma((3, PARTS)), dma((6,))],
            compiler_params=pltpu.CompilerParams(vmem_limit_bytes=VMEM_B),
            cost_estimate=pl.CostEstimate(flops=10_000_000, bytes_accessed=10_000_000, transcendentals=0),
            name="apply_update",
        )(*mid)
        return tuple(out)

    act_spec = P(None, "row")
    cot_spec = P(None, "col")
    w_spec = P("row", "col")
    r_spec = P("row")
    c_spec = P("col")
    s_spec = P()
    return jax.shard_map(local_program, mesh=mesh, in_specs=(act_spec, act_spec, cot_spec, cot_spec, cot_spec, w_spec, w_spec, w_spec, r_spec, c_spec, r_spec, c_spec, r_spec, c_spec, s_spec, s_spec, s_spec), out_specs=(w_spec, w_spec, w_spec, r_spec, c_spec, r_spec, c_spec, r_spec, c_spec), check_vma=False)
```

```python
import functools

import jax
import jax.numpy as jnp
from jax import lax
from jax.experimental import pallas as pl
from jax.experimental.pallas import tpu as pltpu
from jax.sharding import PartitionSpec as P

F32 = jnp.float32
BF16 = jnp.bfloat16
MESH = pl.DeviceIdType.MESH
EPS_SQ = 1e-30
EPS_SCALE = 1e-3
LANES = 128
SUBLANES = 8
GATE_CHUNKS = 2
UP_CHUNKS = 2
CONTRACT_TOKENS = (((0,), (0,)), ((), ()))
VMEM_SPEC = pl.BlockSpec(memory_space=pltpu.VMEM)
HBM_SPEC = pl.BlockSpec(memory_space=pltpu.HBM)
SMEM_SPEC = pl.BlockSpec(memory_space=pltpu.SMEM)
VMEM_A = 44 * 2**20
VMEM_B = 14 * 2**20


def token_dot(act, cot):
    return lax.dot_general(act, cot, CONTRACT_TOKENS, preferred_element_type=F32)


def tree_sum(parts):
    while len(parts) > 1:
        parts = [sum(parts[k + 1 : k + 2], parts[k]) for k in range(0, len(parts), 2)]
    return parts[0]


def lane_groups(value):
    return tree_sum([value[:, k : k + LANES] for k in range(0, value.shape[1], LANES)])


def row_groups(value):
    return tree_sum([value[k : k + SUBLANES] for k in range(0, value.shape[0], SUBLANES)])


def tile_rows(ref):
    return 64 if ref.shape[1] > 1024 else 128


def over_rows(ref, body, init):
    size = tile_rows(ref)
    return lax.fori_loop(0, ref.shape[0] // size, lambda i, carry: body(pl.ds(pl.multiple_of(i * size, size), size), carry), init)


def update_kernel(row_count, col_count, x_hbm, h_hbm, dg_hbm, du_hbm, do_hbm, wg_hbm, wu_hbm, wd_hbm, rg, cg, ru, cu, rd, cd, beta_ref, step_ref, clip_ref,
                  g_gate, g_up, g_down, w_gate, w_up, w_down, a_gate, a_up, a_down, b_gate, b_up, b_down, rn_gate, cn_gate, rn_up, cn_up, rn_down, cn_down,
                  x_buf, gate_buf, mix_buf, row_gate, row_up, row_down, col_gate, col_up, col_down, tail_buf,
                  old_gate_r, old_gate_c, old_up_r, old_up_c, old_down_r, old_down_c, load_sem, w_sem, small_sem, row_send, row_recv, col_send, col_recv, tail_send, tail_recv):
    row_me = lax.axis_index("row")
    col_me = lax.axis_index("col")
    plane = row_count * col_count
    tokens = x_hbm.shape[0]
    h_cols = h_hbm.shape[1]
    do_cols = do_hbm.shape[1]

    def row_peer(k):
        return lax.rem(row_me + k, row_count)

    def col_peer(k):
        return lax.rem(col_me + k, col_count)

    def farthest_first(count):
        return sorted(range(1, count), key=lambda k: -min(k, count - k))

    def plane_peers():
        offsets = [(dc, dr) for dc in range(col_count) for dr in range(row_count) if dc or dr]
        offsets.sort(key=lambda o: -min(o[0], col_count - o[0]) - min(o[1], row_count - o[1]) / 2)
        return [{"col": col_peer(dc), "row": row_peer(dr)} for dc, dr in offsets]

    def start(copies):
        for copy in copies:
            copy.start()

    def wait(copies):
        for copy in copies:
            copy.wait()

    def rows(i, count):
        return pl.ds(pl.multiple_of(i * (tokens // count), tokens // count), tokens // count)

    def load(src, dst, s, kind, i):
        return pltpu.make_async_copy(src.at[s, :], dst, load_sem.at[kind, i])

    def head_rows(i, count=None):
        return rows(i, 8)

    def rest_rows(i, count=None):
        size = 3 * tokens // 8
        return pl.ds(pl.multiple_of(tokens // 4 + i * size, tokens // 8), size)

    def down_load_pair(s, kind, i):
        return [load(h_hbm, mix_buf.at[s, pl.ds(0, h_cols)], s, kind, i), load(do_hbm, mix_buf.at[s, pl.ds(h_cols, do_cols)], s, kind + 1, i)]

    def head_loads(i):
        return down_load_pair(head_rows(i), 0, i)

    def rest_loads(i):
        return down_load_pair(rest_rows(i), 5, i)

    def gate_loads(i):
        s = rows(i, GATE_CHUNKS)
        return [load(x_hbm, x_buf.at[s, :], s, 2, i), load(dg_hbm, gate_buf.at[s, :], s, 3, i)]

    def up_loads(i):
        s = rows(i, UP_CHUNKS)
        return [load(du_hbm, mix_buf.at[s, :], s, 4, i)]

    w_copies = [pltpu.make_async_copy(src, dst, w_sem.at[k]) for k, (src, dst) in enumerate(((wd_hbm, w_down), (wg_hbm, w_gate), (wu_hbm, w_up)))]
    stat_copies = [pltpu.make_async_copy(src, dst, small_sem.at[k]) for k, (src, dst) in enumerate(((rg, old_gate_r), (cg, old_gate_c), (ru, old_up_r), (cu, old_up_c), (rd, old_down_r), (cd, old_down_c)))]

    def exchange(kind, buf, own, send_sem, recv_sem, index):
        count, me, peer = (col_count, col_me, col_peer) if kind == "col" else (row_count, row_me, row_peer)
        buf[pl.ds(me, 1)] = own[None]
        for k in farthest_first(count):
            pltpu.make_async_remote_copy(buf.at[me], buf.at[me], send_sem.at[index], recv_sem.at[index], device_id={kind: peer(k)}, device_id_type=MESH).start()

        def finish():
            for sem in (send_sem, recv_sem):
                pltpu.make_async_copy(buf.at[pl.ds(0, count - 1)], buf.at[pl.ds(0, count - 1)], sem.at[index]).wait()
        return finish

    def block_sums(g_ref, lane_ref, s, columns):
        g = g_ref[s, :]
        q = g * g
        lane_ref[s, :] = lane_groups(q)
        return columns + row_groups(q)

    def no_columns(g_ref):
        return jnp.zeros((SUBLANES, g_ref.shape[1]), F32)

    def send_sums(columns, g_ref, lane_ref, row_buf, col_buf, index):
        col_part = jnp.sum(columns, axis=0, keepdims=True) + g_ref.shape[0] * EPS_SQ
        row_part = jnp.sum(lane_ref[...].T, axis=0, keepdims=True) + g_ref.shape[1] * EPS_SQ
        first = exchange("row", col_buf, col_part, col_send, col_recv, index)
        second = exchange("col", row_buf, row_part, row_send, row_recv, index)
        return first, second

    def new_stats(finish, g_ref, row_buf, col_buf, r_old, c_old, r_new, c_new, a_ref, b_ref):
        finish_columns, finish_rows = finish
        finish_rows()
        m_total = g_ref.shape[0] * row_count
        n_total = g_ref.shape[1] * col_count
        beta = beta_ref[...]
        row_sum = tree_sum([row_buf[k] for k in range(col_count)])
        r_val = beta * r_old[...].reshape(1, -1) + (1.0 - beta) * (row_sum / n_total)
        r_new[...] = r_val.reshape(-1)
        a_row = 1.0 / jnp.sqrt(r_val)
        a_ref[...] = jnp.broadcast_to(a_row, (LANES, a_row.shape[1])).T
        finish_columns()
        col_sum = tree_sum([col_buf[k] for k in range(row_count)])
        c_val = beta * c_old[...].reshape(1, -1) + (1.0 - beta) * (col_sum / m_total)
        c_new[...] = c_val.reshape(-1)
        b_ref[...] = 1.0 / jnp.sqrt(c_val)

        def body(s, total):
            t = g_ref[s, :] * b_ref[...]
            u = lane_groups(t * t) * (a_ref[s, :] * a_ref[s, :])
            return total + row_groups(u)

        return over_rows(g_ref, body, jnp.zeros((SUBLANES, LANES), F32)), lane_groups(r_val)

    def square_sum(w_ref):
        def body(s, total):
            w = w_ref[s, :]
            return total + row_groups(lane_groups(w * w))

        return over_rows(w_ref, body, jnp.zeros((SUBLANES, LANES), F32))

    def matmul(g_ref, count, loads, act, cot, beside, init, pick=rows, clear=True):
        def step(i, carry):
            wait(loads(i))
            carry = beside(i, carry)
            s = pick(i, count)
            product = token_dot(act(s), cot(s))
            g_ref[...] = (jnp.where(i == 0, 0.0, g_ref[...]) if clear else g_ref[...]) + product
            return carry

        return lax.fori_loop(0, count, step, init)

    for i in range(2):
        start(head_loads(i))
    for i in range(2):
        start(rest_loads(i))
    for i in range(GATE_CHUNKS):
        start(gate_loads(i))
    barrier = pltpu.get_barrier_semaphore()
    for peer in plane_peers():
        pl.semaphore_signal(barrier, inc=1, device_id=peer, device_id_type=MESH)
    down_act = lambda s: mix_buf[s, 0:h_cols]
    down_cot = lambda s: mix_buf[s, h_cols : h_cols + do_cols]
    matmul(g_down, 2, head_loads, down_act, down_cot, lambda i, c: c, 0, head_rows)
    matmul(g_down, 2, rest_loads, down_act, down_cot, lambda i, c: c, 0, rest_rows, False)
    for i in range(UP_CHUNKS):
        start(up_loads(i))
    start(w_copies)
    start(stat_copies)
    pl.semaphore_wait(barrier, plane - 1)

    def down_sums(i, columns):
        size = g_down.shape[0] // GATE_CHUNKS
        return block_sums(g_down, a_down, pl.ds(pl.multiple_of(i * size, size), size), columns)

    columns = matmul(g_gate, GATE_CHUNKS, gate_loads, lambda s: x_buf[s, :], lambda s: gate_buf[s, :], down_sums, no_columns(g_down))
    down_out = send_sums(columns, g_down, a_down, row_down, col_down, 0)
    columns = over_rows(g_gate, lambda s, c: block_sums(g_gate, a_gate, s, c), no_columns(g_gate))
    gate_out = send_sums(columns, g_gate, a_gate, row_gate, col_gate, 1)

    matmul(g_up, UP_CHUNKS, up_loads, lambda s: x_buf[s, :], lambda s: mix_buf[s, :], lambda i, c: c, 0)
    columns = over_rows(g_up, lambda s, c: block_sums(g_up, a_up, s, c), no_columns(g_up))
    up_out = send_sums(columns, g_up, a_up, row_up, col_up, 2)

    wait(w_copies)
    wait(stat_copies)
    w_sums = [square_sum(w) for w in (w_down, w_gate, w_up)]
    u_down, r_down = new_stats(down_out, g_down, row_down, col_down, old_down_r, old_down_c, rn_down, cn_down, a_down, b_down)
    u_gate, r_gate = new_stats(gate_out, g_gate, row_gate, col_gate, old_gate_r, old_gate_c, rn_gate, cn_gate, a_gate, b_gate)
    u_up, r_up = new_stats(up_out, g_up, row_up, col_up, old_up_r, old_up_c, rn_up, cn_up, a_up, b_up)

    lane = lax.broadcasted_iota(jnp.int32, (1, LANES), 1)
    packed = jnp.zeros((1, LANES), F32)
    for k, value in enumerate(w_sums + [r_down, r_gate, r_up, u_down, u_gate, u_up]):
        packed = jnp.where(lane == k, jnp.sum(jnp.sum(value, axis=0, keepdims=True), axis=1, keepdims=True), packed)
    me = col_me * row_count + row_me
    tail_buf[pl.ds(me, 1)] = packed[None]
    for peer in plane_peers():
        pltpu.make_async_remote_copy(tail_buf.at[me], tail_buf.at[me], tail_send, tail_recv, device_id=peer, device_id_type=MESH).start()
    for sem in (tail_send, tail_recv):
        pltpu.make_async_copy(tail_buf.at[pl.ds(0, plane - 1)], tail_buf.at[pl.ds(0, plane - 1)], sem).wait()
    sums = jnp.sum(tail_buf[...], axis=0)

    def pick(k):
        return jnp.sum(jnp.where(lane == k, sums, 0.0), axis=1, keepdims=True)

    for k, (g_ref, a_ref) in enumerate(((g_down, a_down), (g_gate, a_gate), (g_up, a_up))):
        m_total = g_ref.shape[0] * row_count
        n_total = g_ref.shape[1] * col_count
        r_mean = pick(3 + k) / (m_total * col_count)
        w_rms = jnp.sqrt(pick(k) / (m_total * n_total))
        u_rms = jnp.sqrt(r_mean * pick(6 + k) / (m_total * n_total))
        size = step_ref[...] * jnp.maximum(EPS_SCALE, w_rms)
        scale = size * jnp.sqrt(r_mean) / jnp.maximum(1.0, u_rms / clip_ref[...])
        a_ref[...] = a_ref[...] * scale


PARTS = 4


def apply_kernel(g_gate, g_up, g_down, w_gate, w_up, w_down, a_gate, a_up, a_down, b_gate, b_up, b_down, rn_gate, cn_gate, rn_up, cn_up, rn_down, cn_down,
                 o_gate, o_up, o_down, ro_gate, co_gate, ro_up, co_up, ro_down, co_down, t_gate, t_up, t_down, w_sem, s_sem):
    small = [pltpu.make_async_copy(src, dst, s_sem.at[k]) for k, (src, dst) in enumerate(((rn_gate, ro_gate), (cn_gate, co_gate), (rn_up, ro_up), (cn_up, co_up), (rn_down, ro_down), (cn_down, co_down)))]
    for copy in small:
        copy.start()
    blocks = ((g_down, w_down, a_down, b_down, t_down, o_down), (g_gate, w_gate, a_gate, b_gate, t_gate, o_gate), (g_up, w_up, a_up, b_up, t_up, o_up))

    def out_copy(k, i):
        t, o = blocks[k][4:]
        size = t.shape[0] // PARTS
        s = pl.ds(pl.multiple_of(i * size, size), size)
        return pltpu.make_async_copy(t.at[s, :], o.at[s, :], w_sem.at[k, i])

    for k, (g, w, a, b, t, o) in enumerate(blocks):
        size = g.shape[0] // PARTS
        tile = min(tile_rows(g) // 2, size)

        def part(i, carry):
            def body(j, inner):
                s = pl.ds(pl.multiple_of(i * size + j * tile, tile), tile)
                a_val = a[s, :]
                for c in range(0, g.shape[1], LANES):
                    ls = pl.ds(c, LANES)
                    t[s, ls] = w[s, ls] - g[s, ls] * (a_val * b[:, ls])
                return inner

            lax.fori_loop(0, size // tile, body, 0)
            out_copy(k, i).start()
            return carry

        lax.fori_loop(0, PARTS, part, 0)
    for k in range(len(blocks)):
        for i in range(PARTS):
            out_copy(k, i).wait()
    for copy in small:
        copy.wait()


def solution(mesh):
    row_count = mesh.shape["row"]
    col_count = mesh.shape["col"]

    def local_program(x_in, h_act, d_gate, d_up, d_out, w_gate, w_up, w_down, r_gate, c_gate, r_up, c_up, r_down, c_down, beta_two, rel_step, clip_thr):
        blocks = (w_gate, w_up, w_down)
        tokens = x_in.shape[0]
        out_shape = [pltpu.VMEM(w.shape, F32) for w in blocks] * 2
        out_shape += [pltpu.VMEM((w.shape[0], LANES), F32) for w in blocks]
        out_shape += [pltpu.VMEM((1, w.shape[1]), F32) for w in blocks]
        stats = [pltpu.VMEM((w.shape[k],), F32) for w in blocks for k in range(2)]
        dma = pltpu.SemaphoreType.DMA
        flops = sum(2 * tokens * w.shape[0] * w.shape[1] for w in blocks)
        mid = pl.pallas_call(
            functools.partial(update_kernel, row_count, col_count),
            out_shape=out_shape + stats,
            in_specs=[HBM_SPEC] * 14 + [SMEM_SPEC] * 3,
            out_specs=[VMEM_SPEC] * 18,
            scratch_shapes=[
                pltpu.VMEM(x_in.shape, BF16),
                pltpu.VMEM(d_gate.shape, BF16),
                pltpu.VMEM((tokens, max(d_up.shape[1], h_act.shape[1] + d_out.shape[1])), BF16),
                *[pltpu.VMEM((col_count, 1, w.shape[0]), F32) for w in blocks],
                *[pltpu.VMEM((row_count, 1, w.shape[1]), F32) for w in blocks],
                pltpu.VMEM((row_count * col_count, 1, LANES), F32),
                *[pltpu.VMEM((w.shape[k],), F32) for w in blocks for k in range(2)],
                dma((7, 4)), dma((3,)), dma((6,)), dma((3,)), dma((3,)), dma((3,)), dma((3,)), dma, dma,
            ],
            compiler_params=pltpu.CompilerParams(collective_id=0, has_side_effects=True, vmem_limit_bytes=VMEM_A),
            cost_estimate=pl.CostEstimate(flops=flops, bytes_accessed=60_000_000, transcendentals=0),
            name="grad_and_stats",
        )(x_in, h_act, d_gate, d_up, d_out, w_gate, w_up, w_down, r_gate, c_gate, r_up, c_up, r_down, c_down, beta_two, rel_step, clip_thr)
        out = pl.pallas_call(
            apply_kernel,
            out_shape=[jax.ShapeDtypeStruct(w.shape, F32) for w in blocks] + [jax.ShapeDtypeStruct((w.shape[k],), F32) for w in blocks for k in range(2)],
            in_specs=[VMEM_SPEC] * 18,
            out_specs=[HBM_SPEC] * 9,
            scratch_shapes=[pltpu.VMEM(w.shape, F32) for w in blocks] + [dma((3, PARTS)), dma((6,))],
            compiler_params=pltpu.CompilerParams(vmem_limit_bytes=VMEM_B),
            cost_estimate=pl.CostEstimate(flops=10_000_000, bytes_accessed=10_000_000, transcendentals=0),
            name="apply_update",
        )(*mid)
        return tuple(out)

    act_spec = P(None, "row")
    cot_spec = P(None, "col")
    w_spec = P("row", "col")
    r_spec = P("row")
    c_spec = P("col")
    s_spec = P()
    return jax.shard_map(local_program, mesh=mesh, in_specs=(act_spec, act_spec, cot_spec, cot_spec, cot_spec, w_spec, w_spec, w_spec, r_spec, c_spec, r_spec, c_spec, r_spec, c_spec, s_spec, s_spec, s_spec), out_specs=(w_spec, w_spec, w_spec, r_spec, c_spec, r_spec, c_spec, r_spec, c_spec), check_vma=False)
```

```python
import functools

import jax
import jax.numpy as jnp
from jax import lax
from jax.experimental import pallas as pl
from jax.experimental.pallas import tpu as pltpu
from jax.sharding import PartitionSpec as P

F32 = jnp.float32
BF16 = jnp.bfloat16
MESH = pl.DeviceIdType.MESH
EPS_SQ = 1e-30
EPS_SCALE = 1e-3
LANES = 128
SUBLANES = 8
GATE_CHUNKS = 2
UP_CHUNKS = 2
CONTRACT_TOKENS = (((0,), (0,)), ((), ()))
VMEM_SPEC = pl.BlockSpec(memory_space=pltpu.VMEM)
HBM_SPEC = pl.BlockSpec(memory_space=pltpu.HBM)
SMEM_SPEC = pl.BlockSpec(memory_space=pltpu.SMEM)
VMEM_A = 44 * 2**20
VMEM_B = 14 * 2**20


def token_dot(act, cot):
    return lax.dot_general(act, cot, CONTRACT_TOKENS, preferred_element_type=F32)


def tree_sum(parts):
    while len(parts) > 1:
        parts = [sum(parts[k + 1 : k + 2], parts[k]) for k in range(0, len(parts), 2)]
    return parts[0]


def lane_groups(value):
    return tree_sum([value[:, k : k + LANES] for k in range(0, value.shape[1], LANES)])


def row_groups(value):
    return tree_sum([value[k : k + SUBLANES] for k in range(0, value.shape[0], SUBLANES)])


def tile_rows(ref):
    return 128 if ref.shape[1] > 1024 else 256


def over_rows(ref, body, init):
    size = tile_rows(ref)
    return lax.fori_loop(0, ref.shape[0] // size, lambda i, carry: body(pl.ds(pl.multiple_of(i * size, size), size), carry), init)


def update_kernel(row_count, col_count, x_hbm, h_hbm, dg_hbm, du_hbm, do_hbm, wg_hbm, wu_hbm, wd_hbm, rg, cg, ru, cu, rd, cd, beta_ref, step_ref, clip_ref,
                  g_gate, g_up, g_down, w_gate, w_up, w_down, a_gate, a_up, a_down, b_gate, b_up, b_down, rn_gate, cn_gate, rn_up, cn_up, rn_down, cn_down,
                  x_buf, gate_buf, mix_buf, row_gate, row_up, row_down, col_gate, col_up, col_down, tail_buf,
                  old_gate_r, old_gate_c, old_up_r, old_up_c, old_down_r, old_down_c, load_sem, w_sem, small_sem, row_send, row_recv, col_send, col_recv, tail_send, tail_recv):
    row_me = lax.axis_index("row")
    col_me = lax.axis_index("col")
    plane = row_count * col_count
    tokens = x_hbm.shape[0]
    h_cols = h_hbm.shape[1]
    do_cols = do_hbm.shape[1]

    def row_peer(k):
        return lax.rem(row_me + k, row_count)

    def col_peer(k):
        return lax.rem(col_me + k, col_count)

    def farthest_first(count):
        return sorted(range(1, count), key=lambda k: -min(k, count - k))

    def plane_peers():
        offsets = [(dc, dr) for dc in range(col_count) for dr in range(row_count) if dc or dr]
        offsets.sort(key=lambda o: -min(o[0], col_count - o[0]) - min(o[1], row_count - o[1]) / 2)
        return [{"col": col_peer(dc), "row": row_peer(dr)} for dc, dr in offsets]

    def start(copies):
        for copy in copies:
            copy.start()

    def wait(copies):
        for copy in copies:
            copy.wait()

    def rows(i, count):
        return pl.ds(pl.multiple_of(i * (tokens // count), tokens // count), tokens // count)

    def load(src, dst, s, kind, i):
        return pltpu.make_async_copy(src.at[s, :], dst, load_sem.at[kind, i])

    def head_rows(i, count=None):
        return rows(i, 8)

    def rest_rows(i, count=None):
        size = 3 * tokens // 8
        return pl.ds(pl.multiple_of(tokens // 4 + i * size, tokens // 8), size)

    def down_load_pair(s, kind, i):
        return [load(h_hbm, mix_buf.at[s, pl.ds(0, h_cols)], s, kind, i), load(do_hbm, mix_buf.at[s, pl.ds(h_cols, do_cols)], s, kind + 1, i)]

    def head_loads(i):
        return down_load_pair(head_rows(i), 0, i)

    def rest_loads(i):
        return down_load_pair(rest_rows(i), 5, i)

    def gate_loads(i):
        s = rows(i, GATE_CHUNKS)
        return [load(x_hbm, x_buf.at[s, :], s, 2, i), load(dg_hbm, gate_buf.at[s, :], s, 3, i)]

    def up_loads(i):
        s = rows(i, UP_CHUNKS)
        return [load(du_hbm, mix_buf.at[s, :], s, 4, i)]

    w_copies = [pltpu.make_async_copy(src, dst, w_sem.at[k]) for k, (src, dst) in enumerate(((wd_hbm, w_down), (wg_hbm, w_gate), (wu_hbm, w_up)))]
    stat_copies = [pltpu.make_async_copy(src, dst, small_sem.at[k]) for k, (src, dst) in enumerate(((rg, old_gate_r), (cg, old_gate_c), (ru, old_up_r), (cu, old_up_c), (rd, old_down_r), (cd, old_down_c)))]

    def exchange(kind, buf, own, send_sem, recv_sem, index):
        count, me, peer = (col_count, col_me, col_peer) if kind == "col" else (row_count, row_me, row_peer)
        buf[pl.ds(me, 1)] = own[None]
        for k in farthest_first(count):
            pltpu.make_async_remote_copy(buf.at[me], buf.at[me], send_sem.at[index], recv_sem.at[index], device_id={kind: peer(k)}, device_id_type=MESH).start()

        def finish():
            for sem in (send_sem, recv_sem):
                pltpu.make_async_copy(buf.at[pl.ds(0, count - 1)], buf.at[pl.ds(0, count - 1)], sem.at[index]).wait()
        return finish

    def block_sums(g_ref, lane_ref, s, columns):
        g = g_ref[s, :]
        q = g * g
        lane_ref[s, :] = lane_groups(q)
        return columns + row_groups(q)

    def no_columns(g_ref):
        return jnp.zeros((SUBLANES, g_ref.shape[1]), F32)

    def send_sums(columns, g_ref, lane_ref, row_buf, col_buf, index):
        col_part = jnp.sum(columns, axis=0, keepdims=True) + g_ref.shape[0] * EPS_SQ
        row_part = jnp.sum(lane_ref[...].T, axis=0, keepdims=True) + g_ref.shape[1] * EPS_SQ
        first = exchange("row", col_buf, col_part, col_send, col_recv, index)
        second = exchange("col", row_buf, row_part, row_send, row_recv, index)
        return first, second

    def new_stats(finish, g_ref, row_buf, col_buf, r_old, c_old, r_new, c_new, a_ref, b_ref):
        finish_columns, finish_rows = finish
        finish_rows()
        m_total = g_ref.shape[0] * row_count
        n_total = g_ref.shape[1] * col_count
        beta = beta_ref[...]
        row_sum = tree_sum([row_buf[k] for k in range(col_count)])
        r_val = beta * r_old[...].reshape(1, -1) + (1.0 - beta) * (row_sum / n_total)
        r_new[...] = r_val.reshape(-1)
        a_row = 1.0 / jnp.sqrt(r_val)
        a_ref[...] = jnp.broadcast_to(a_row, (LANES, a_row.shape[1])).T
        finish_columns()
        col_sum = tree_sum([col_buf[k] for k in range(row_count)])
        c_val = beta * c_old[...].reshape(1, -1) + (1.0 - beta) * (col_sum / m_total)
        c_new[...] = c_val.reshape(-1)
        b_ref[...] = 1.0 / jnp.sqrt(c_val)

        def body(s, total):
            t = g_ref[s, :] * b_ref[...]
            u = lane_groups(t * t) * (a_ref[s, :] * a_ref[s, :])
            return total + row_groups(u)

        return over_rows(g_ref, body, jnp.zeros((SUBLANES, LANES), F32)), lane_groups(r_val)

    def square_sum(w_ref):
        def body(s, total):
            w = w_ref[s, :]
            return total + row_groups(lane_groups(w * w))

        return over_rows(w_ref, body, jnp.zeros((SUBLANES, LANES), F32))

    def matmul(g_ref, count, loads, act, cot, beside, init, pick=rows, clear=True):
        def step(i, carry):
            wait(loads(i))
            carry = beside(i, carry)
            s = pick(i, count)
            product = token_dot(act(s), cot(s))
            g_ref[...] = (jnp.where(i == 0, 0.0, g_ref[...]) if clear else g_ref[...]) + product
            return carry

        return lax.fori_loop(0, count, step, init)

    for i in range(2):
        start(head_loads(i))
    for i in range(2):
        start(rest_loads(i))
    for i in range(GATE_CHUNKS):
        start(gate_loads(i))
    barrier = pltpu.get_barrier_semaphore()
    for peer in plane_peers():
        pl.semaphore_signal(barrier, inc=1, device_id=peer, device_id_type=MESH)
    down_act = lambda s: mix_buf[s, 0:h_cols]
    down_cot = lambda s: mix_buf[s, h_cols : h_cols + do_cols]
    matmul(g_down, 2, head_loads, down_act, down_cot, lambda i, c: c, 0, head_rows)
    matmul(g_down, 2, rest_loads, down_act, down_cot, lambda i, c: c, 0, rest_rows, False)
    for i in range(UP_CHUNKS):
        start(up_loads(i))
    start(w_copies)
    start(stat_copies)
    pl.semaphore_wait(barrier, plane - 1)

    def down_sums(i, columns):
        size = g_down.shape[0] // GATE_CHUNKS
        return block_sums(g_down, a_down, pl.ds(pl.multiple_of(i * size, size), size), columns)

    columns = matmul(g_gate, GATE_CHUNKS, gate_loads, lambda s: x_buf[s, :], lambda s: gate_buf[s, :], down_sums, no_columns(g_down))
    down_out = send_sums(columns, g_down, a_down, row_down, col_down, 0)
    columns = over_rows(g_gate, lambda s, c: block_sums(g_gate, a_gate, s, c), no_columns(g_gate))
    gate_out = send_sums(columns, g_gate, a_gate, row_gate, col_gate, 1)

    matmul(g_up, UP_CHUNKS, up_loads, lambda s: x_buf[s, :], lambda s: mix_buf[s, :], lambda i, c: c, 0)
    columns = over_rows(g_up, lambda s, c: block_sums(g_up, a_up, s, c), no_columns(g_up))
    up_out = send_sums(columns, g_up, a_up, row_up, col_up, 2)

    wait(w_copies)
    wait(stat_copies)
    w_sums = [square_sum(w) for w in (w_down, w_gate, w_up)]
    u_down, r_down = new_stats(down_out, g_down, row_down, col_down, old_down_r, old_down_c, rn_down, cn_down, a_down, b_down)
    u_gate, r_gate = new_stats(gate_out, g_gate, row_gate, col_gate, old_gate_r, old_gate_c, rn_gate, cn_gate, a_gate, b_gate)
    u_up, r_up = new_stats(up_out, g_up, row_up, col_up, old_up_r, old_up_c, rn_up, cn_up, a_up, b_up)

    lane = lax.broadcasted_iota(jnp.int32, (1, LANES), 1)
    packed = jnp.zeros((1, LANES), F32)
    for k, value in enumerate(w_sums + [r_down, r_gate, r_up, u_down, u_gate, u_up]):
        packed = jnp.where(lane == k, jnp.sum(jnp.sum(value, axis=0, keepdims=True), axis=1, keepdims=True), packed)
    me = col_me * row_count + row_me
    tail_buf[pl.ds(me, 1)] = packed[None]
    for peer in plane_peers():
        pltpu.make_async_remote_copy(tail_buf.at[me], tail_buf.at[me], tail_send, tail_recv, device_id=peer, device_id_type=MESH).start()
    for sem in (tail_send, tail_recv):
        pltpu.make_async_copy(tail_buf.at[pl.ds(0, plane - 1)], tail_buf.at[pl.ds(0, plane - 1)], sem).wait()
    sums = jnp.sum(tail_buf[...], axis=0)

    def pick(k):
        return jnp.sum(jnp.where(lane == k, sums, 0.0), axis=1, keepdims=True)

    for k, (g_ref, a_ref) in enumerate(((g_down, a_down), (g_gate, a_gate), (g_up, a_up))):
        m_total = g_ref.shape[0] * row_count
        n_total = g_ref.shape[1] * col_count
        r_mean = pick(3 + k) / (m_total * col_count)
        w_rms = jnp.sqrt(pick(k) / (m_total * n_total))
        u_rms = jnp.sqrt(r_mean * pick(6 + k) / (m_total * n_total))
        size = step_ref[...] * jnp.maximum(EPS_SCALE, w_rms)
        scale = size * jnp.sqrt(r_mean) / jnp.maximum(1.0, u_rms / clip_ref[...])
        a_ref[...] = a_ref[...] * scale


PARTS = 4


def apply_kernel(g_gate, g_up, g_down, w_gate, w_up, w_down, a_gate, a_up, a_down, b_gate, b_up, b_down, rn_gate, cn_gate, rn_up, cn_up, rn_down, cn_down,
                 o_gate, o_up, o_down, ro_gate, co_gate, ro_up, co_up, ro_down, co_down, t_gate, t_up, t_down, w_sem, s_sem):
    small = [pltpu.make_async_copy(src, dst, s_sem.at[k]) for k, (src, dst) in enumerate(((rn_gate, ro_gate), (cn_gate, co_gate), (rn_up, ro_up), (cn_up, co_up), (rn_down, ro_down), (cn_down, co_down)))]
    for copy in small:
        copy.start()
    blocks = ((g_down, w_down, a_down, b_down, t_down, o_down), (g_gate, w_gate, a_gate, b_gate, t_gate, o_gate), (g_up, w_up, a_up, b_up, t_up, o_up))

    def out_copy(k, i):
        t, o = blocks[k][4:]
        size = t.shape[0] // PARTS
        s = pl.ds(pl.multiple_of(i * size, size), size)
        return pltpu.make_async_copy(t.at[s, :], o.at[s, :], w_sem.at[k, i])

    for k, (g, w, a, b, t, o) in enumerate(blocks):
        size = g.shape[0] // PARTS
        tile = min(tile_rows(g) // 4, size)

        def part(i, carry):
            def body(j, inner):
                s = pl.ds(pl.multiple_of(i * size + j * tile, tile), tile)
                a_val = a[s, :]
                for c in range(0, g.shape[1], LANES):
                    ls = pl.ds(c, LANES)
                    t[s, ls] = w[s, ls] - g[s, ls] * (a_val * b[:, ls])
                return inner

            lax.fori_loop(0, size // tile, body, 0)
            out_copy(k, i).start()
            return carry

        lax.fori_loop(0, PARTS, part, 0)
    for k in range(len(blocks)):
        for i in range(PARTS):
            out_copy(k, i).wait()
    for copy in small:
        copy.wait()


def solution(mesh):
    row_count = mesh.shape["row"]
    col_count = mesh.shape["col"]

    def local_program(x_in, h_act, d_gate, d_up, d_out, w_gate, w_up, w_down, r_gate, c_gate, r_up, c_up, r_down, c_down, beta_two, rel_step, clip_thr):
        blocks = (w_gate, w_up, w_down)
        tokens = x_in.shape[0]
        out_shape = [pltpu.VMEM(w.shape, F32) for w in blocks] * 2
        out_shape += [pltpu.VMEM((w.shape[0], LANES), F32) for w in blocks]
        out_shape += [pltpu.VMEM((1, w.shape[1]), F32) for w in blocks]
        stats = [pltpu.VMEM((w.shape[k],), F32) for w in blocks for k in range(2)]
        dma = pltpu.SemaphoreType.DMA
        flops = sum(2 * tokens * w.shape[0] * w.shape[1] for w in blocks)
        mid = pl.pallas_call(
            functools.partial(update_kernel, row_count, col_count),
            out_shape=out_shape + stats,
            in_specs=[HBM_SPEC] * 14 + [SMEM_SPEC] * 3,
            out_specs=[VMEM_SPEC] * 18,
            scratch_shapes=[
                pltpu.VMEM(x_in.shape, BF16),
                pltpu.VMEM(d_gate.shape, BF16),
                pltpu.VMEM((tokens, max(d_up.shape[1], h_act.shape[1] + d_out.shape[1])), BF16),
                *[pltpu.VMEM((col_count, 1, w.shape[0]), F32) for w in blocks],
                *[pltpu.VMEM((row_count, 1, w.shape[1]), F32) for w in blocks],
                pltpu.VMEM((row_count * col_count, 1, LANES), F32),
                *[pltpu.VMEM((w.shape[k],), F32) for w in blocks for k in range(2)],
                dma((7, 4)), dma((3,)), dma((6,)), dma((3,)), dma((3,)), dma((3,)), dma((3,)), dma, dma,
            ],
            compiler_params=pltpu.CompilerParams(collective_id=0, has_side_effects=True, vmem_limit_bytes=VMEM_A),
            cost_estimate=pl.CostEstimate(flops=flops, bytes_accessed=60_000_000, transcendentals=0),
            name="grad_and_stats",
        )(x_in, h_act, d_gate, d_up, d_out, w_gate, w_up, w_down, r_gate, c_gate, r_up, c_up, r_down, c_down, beta_two, rel_step, clip_thr)
        out = pl.pallas_call(
            apply_kernel,
            out_shape=[jax.ShapeDtypeStruct(w.shape, F32) for w in blocks] + [jax.ShapeDtypeStruct((w.shape[k],), F32) for w in blocks for k in range(2)],
            in_specs=[VMEM_SPEC] * 18,
            out_specs=[HBM_SPEC] * 9,
            scratch_shapes=[pltpu.VMEM(w.shape, F32) for w in blocks] + [dma((3, PARTS)), dma((6,))],
            compiler_params=pltpu.CompilerParams(vmem_limit_bytes=VMEM_B),
            cost_estimate=pl.CostEstimate(flops=10_000_000, bytes_accessed=10_000_000, transcendentals=0),
            name="apply_update",
        )(*mid)
        return tuple(out)

    act_spec = P(None, "row")
    cot_spec = P(None, "col")
    w_spec = P("row", "col")
    r_spec = P("row")
    c_spec = P("col")
    s_spec = P()
    return jax.shard_map(local_program, mesh=mesh, in_specs=(act_spec, act_spec, cot_spec, cot_spec, cot_spec, w_spec, w_spec, w_spec, r_spec, c_spec, r_spec, c_spec, r_spec, c_spec, s_spec, s_spec, s_spec), out_specs=(w_spec, w_spec, w_spec, r_spec, c_spec, r_spec, c_spec, r_spec, c_spec), check_vma=False)
```
